512 devices in a mesh: prompt: 2 (over y), seq: 16 (over z), blk: 8 (over x), cfg: 2 (over core).
Axes of the slice: x: 8, y: 2, z: 16, core: 2. Of those that a mesh axis runs over, the one named last changes fastest.
The devices are a block of a 8x8x16 slice.
Arguments:
- queries: bfloat16 [2, 12288, 4096], P('cfg', ('prompt', 'blk', 'seq')), parts along dimension 1, may hold values from -5 to 5
- key_states: bfloat16 [2, 12288, 4096], P('cfg', ('prompt', 'blk', 'seq')), parts along dimension 1, may hold values from -5 to 5
- value_states: bfloat16 [2, 12288, 4096], P('cfg', ('prompt', 'blk', 'seq')), parts along dimension 1, may hold values from -6 to 6
- noisy_latents: float32 [12288, 64], P(('prompt', 'blk', 'seq')), parts along dimension 0, may hold values from -6 to 6
- patch_order: int32 [12288], P(('prompt', 'blk', 'seq')), parts along dimension 0, may hold values from 0 to 6143, as said below
- head_weight: bfloat16 [4096, 64], replicated, may hold values from -0.75 to 0.75
- latent_std: float32 [16], replicated, may hold values from 0.1 to 1.9
- latent_mean: float32 [16], replicated, may hold values from -3 to 3
- conv_weight: bfloat16 [3, 3, 3, 16, 384], replicated, may hold values from -0.3125 to 0.3125
- conv_bias: float32 [384], replicated, may hold values from -2 to 2
Outputs:
- features: bfloat16 [16, 64, 48, 384], P(('prompt', 'cfg'), 'seq', 'blk'), parts along dimension 0
The draws below stay inside these ranges and needn't reach their ends.
There are 2 independent parts, one for each index of `prompt`. The reference program is written for one: setup_inputs(seed, part) draws one part's arguments, and reference() takes and returns one part's arrays. A program takes and returns all parts, laid end to end along the dimension named above; an argument that names none is the same for every part. Nothing has to cross between parts.
Inputs may be any that keep to these rules, and one draw needn't show every extreme that they name: A permutation of 0 to 6143 that keeps every aligned block of 48 tokens within itself: patch_order[t] // 48 == t // 48.
All inputs are finite; a program needn't handle non-finite values.
Results may differ from the reference program's by a relative error of at most 0.012.
Values may be sent and summed in bfloat16 or wider, within the bound.
A program may use at most 128 MiB of HBM per device.

```python
import math
import jax
import jax.numpy as jnp
from jax import lax

HEADS = 32
HDIM = 128
ZCH = 16
CONV_OUT = 384
PATCH = 64
HD = 4096
FRAMES = 8
HP = 32
WP = 24
TOK_DEV = 48
TOKENS = 6144


def attention_pair(key):
    base = jax.random.fold_in(key, 7)
    key_query, key_keys = jax.random.split(base, 2)
    shape = (2, TOKENS, HEADS * HDIM)
    query_part = jax.random.truncated_normal(key_query, -4.0, 4.0, shape, jnp.float32)
    keys_part = jax.random.truncated_normal(key_keys, -4.0, 4.0, shape, jnp.float32)
    return (query_part, keys_part)


def draw_queries(key, part):
    return attention_pair(key)[0].astype(jnp.bfloat16)


def draw_key_states(key, part):
    return attention_pair(key)[1].astype(jnp.bfloat16)


def draw_patch_order(key, part):
    blocks = TOKENS // TOK_DEV
    subkeys = jax.random.split(jax.random.fold_in(key, 11), blocks)
    orders = jax.vmap(lambda single: jax.random.permutation(single, TOK_DEV))(subkeys)
    offsets = (jnp.arange(blocks, dtype=jnp.int32) * TOK_DEV)[:, None]
    return (orders.astype(jnp.int32) + offsets).reshape(TOKENS).astype(jnp.int32)


def shard_levels(rng, extent, cuts, low, top_value):
    gain, own = 1.0, jax.random.fold_in(rng, 6)
    for axis_at, blocks in cuts:
        draws = jnp.exp(jax.random.uniform(jax.random.fold_in(own, axis_at), (blocks,), jnp.float32, low / len(cuts), top_value / len(cuts)))
        gain = gain * jnp.repeat(draws, extent[axis_at] // blocks).reshape([-1 if axis == axis_at else 1 for axis in range(len(extent))])
    return gain


def normal_values(stream_key, dims, scale, bound, cuts=(), kind=jnp.bfloat16):
    entries = scale * jax.random.normal(stream_key, dims, jnp.float32)
    if cuts:
        entries = entries * shard_levels(stream_key, dims, cuts, -0.22, 0.18)
    return jnp.clip(entries, -bound, bound).astype(kind)


def setup_inputs(seed: int = 0, part: int = 0) -> dict:
    arg_keys = jax.random.split(jax.random.key(seed), 11)
    part_splits = jax.random.split(jax.random.fold_in(arg_keys[10], part), 11)
    queries = draw_queries(jax.random.fold_in(jax.random.fold_in(arg_keys[10], part), 71), part)
    key_states = draw_key_states(jax.random.fold_in(jax.random.fold_in(arg_keys[10], part), 71), part)
    value_states = normal_values(part_splits[2], (2, TOKENS, HD), 1.0, 6.0, ((0, 2), (1, 128)))
    noisy_latents = normal_values(part_splits[3], (TOKENS, PATCH), 1.0, 6.0, ((0, 128),), jnp.float32)
    patch_order = draw_patch_order(jax.random.fold_in(jax.random.fold_in(arg_keys[10], part), 71), part)
    head_weight = normal_values(arg_keys[5], (HD, PATCH), (HD // 64) ** -0.5, 0.75)
    latent_std = jnp.clip(1.0 + 0.18 * jax.random.normal(arg_keys[6], (ZCH,), jnp.float32), 0.1, 1.9)
    latent_mean = normal_values(arg_keys[7], (ZCH,), 0.5, 3.0, (), jnp.float32)
    conv_weight = normal_values(arg_keys[8], (3, 3, 3, ZCH, CONV_OUT), (27 * ZCH) ** -0.5, 0.3125)
    conv_bias = normal_values(arg_keys[9], (CONV_OUT,), 0.3, 2.0, (), jnp.float32)
    return {"queries": queries, "key_states": key_states, "value_states": value_states, "noisy_latents": noisy_latents, "patch_order": patch_order, "head_weight": head_weight, "latent_std": latent_std, "latent_mean": latent_mean, "conv_weight": conv_weight, "conv_bias": conv_bias}


GUIDE = 5.0
NOISE_LEVEL = 0.5

def reference(queries, key_states, value_states, noisy_latents, patch_order, head_weight, latent_std, latent_mean, conv_weight, conv_bias):
    scale = 1.0 / math.sqrt(HDIM)

    def one_head(index):
        branch = (index // HEADS).astype(jnp.int32)
        head = (index % HEADS).astype(jnp.int32)
        start = (jnp.int32(0) * branch, jnp.int32(0) * branch, head * HDIM)
        q_rows = lax.dynamic_slice(queries, (branch, start[1], start[2]), (1, TOKENS, HDIM))[0]
        k_rows = lax.dynamic_slice(key_states, (branch, start[1], start[2]), (1, TOKENS, HDIM))[0]
        v_rows = lax.dynamic_slice(value_states, (branch, start[1], start[2]), (1, TOKENS, HDIM))[0]
        scores = jnp.dot(q_rows, k_rows.T, preferred_element_type=jnp.float32) * scale
        top = lax.optimization_barrier(jnp.max(scores, axis=1, keepdims=True))
        expo = jnp.exp(scores - top)
        total = lax.optimization_barrier(jnp.sum(expo, axis=1, keepdims=True))
        mixed = jnp.dot(expo.astype(jnp.bfloat16), v_rows, preferred_element_type=jnp.float32) / total
        return mixed.astype(jnp.bfloat16)
    heads_out = lax.map(one_head, jnp.arange(2 * HEADS, dtype=jnp.int32))
    attended = heads_out.reshape(2, HEADS, TOKENS, HDIM).transpose(0, 2, 1, 3).reshape(2, TOKENS, HD)
    cond = jnp.dot(attended[0], head_weight, preferred_element_type=jnp.float32)
    uncond = jnp.dot(attended[1], head_weight, preferred_element_type=jnp.float32)
    guided = uncond + GUIDE * (cond - uncond)
    denoised = noisy_latents - NOISE_LEVEL * guided
    pixels = (denoised * jnp.tile(latent_std, 4) + jnp.tile(latent_mean, 4)).astype(jnp.bfloat16)
    placed = jnp.zeros((TOKENS, PATCH), jnp.bfloat16).at[patch_order.astype(jnp.int32)].set(pixels)
    latent_grid = placed.reshape(FRAMES, HP, WP, 2, 2, ZCH).transpose(0, 1, 3, 2, 4, 5).reshape(FRAMES, 2 * HP, 2 * WP, ZCH)
    padded = jnp.pad(latent_grid, ((2, 0), (1, 1), (1, 1), (0, 0)))
    output = jnp.zeros((FRAMES * 2 * HP * 2 * WP, CONV_OUT), jnp.float32)
    for step_t in range(3):
        for step_y in range(3):
            for step_x in range(3):
                window = padded[step_t:step_t + FRAMES, step_y:step_y + 2 * HP, step_x:step_x + 2 * WP, :]
                output = output + jnp.dot(window.reshape(-1, ZCH), conv_weight[step_t, step_y, step_x], preferred_element_type=jnp.float32)
    output = output + conv_bias[None, :]
    return output.reshape(FRAMES, 2 * HP, 2 * WP, CONV_OUT).astype(jnp.bfloat16)
```

```python
import functools
import math

import jax
import jax.numpy as jnp
from jax import lax
from jax.experimental import pallas as pl
from jax.experimental.pallas import tpu as pltpu
from jax.sharding import PartitionSpec as P

HDIM = 128
ZCH = 16
COLS_DEV = 3
GUIDE = 5.0
NOISE_LEVEL = 0.5
MESH = pl.DeviceIdType.MESH
EXP_SCALE = math.log2(math.e) / math.sqrt(HDIM)


def exchange_kernel(
    nz, nx, q_ref, k_ref, v_ref, w_ref, out_ref,
    vsend, gx, qx, vt, top, total, acc, zsend, zrecv, xsend, xrecv,
):
    seq = lax.axis_index("seq")
    blk = lax.axis_index("blk")
    tok = q_ref.shape[0]
    rows = gx.shape[2]
    part = rows // 2
    patch = w_ref.shape[1]
    hops = nx // 2
    right = lax.rem(blk + 1, nx)
    left = lax.rem(blk + nx - 1, nx)

    barrier = pltpu.get_barrier_semaphore()

    def greet(d, _):
        pl.semaphore_signal(
            barrier, inc=1, device_id={"seq": lax.rem(seq + d, nz)}, device_id_type=MESH
        )
        return 0

    lax.fori_loop(1, nz, greet, 0)
    pl.semaphore_signal(barrier, inc=1, device_id={"blk": right}, device_id_type=MESH)
    pl.semaphore_signal(barrier, inc=1, device_id={"blk": left}, device_id_type=MESH)

    def project(s, _):
        both = []
        for h in range(2):
            at = pl.ds(pl.multiple_of((2 * s + h) * HDIM, HDIM), HDIM)
            both.append(
                jnp.dot(v_ref[:, at], w_ref[at, :], preferred_element_type=jnp.float32)
            )
        vsend[s] = jnp.concatenate(both, axis=1).astype(jnp.bfloat16)
        return 0

    lax.fori_loop(0, nz, project, 0)
    pl.semaphore_wait(barrier, nz + 1)

    own_rows = pl.ds(pl.multiple_of(seq * tok, tok), tok)

    def columns(ref, s, h):
        return ref.at[:, pl.ds(pl.multiple_of((2 * s + h) * HDIM, HDIM), HDIM)]

    sources = (
        lambda s: columns(k_ref, s, 0),
        lambda s: vsend.at[s],
        lambda s: columns(q_ref, s, 0),
        lambda s: columns(k_ref, s, 1),
        lambda s: columns(q_ref, s, 1),
    )
    whole = (gx.at[0, blk], gx.at[1, blk], qx.at[0], gx.at[2, blk], qx.at[1])

    def spread(i):
        pltpu.make_async_copy(
            sources[i](seq), whole[i].at[own_rows, :], zrecv.at[i]
        ).start()

        def send(d, _):
            far = (d + 1) // 2
            peer = lax.rem(seq + jnp.where(lax.rem(d, 2) == 1, far, nz - far), nz)
            pltpu.make_async_remote_copy(
                src_ref=sources[i](peer),
                dst_ref=whole[i].at[own_rows, :],
                send_sem=zsend.at[i],
                recv_sem=zrecv.at[i],
                device_id={"seq": peer},
                device_id_type=MESH,
            ).start()
            return 0

        lax.fori_loop(1, nz, send, 0)

    def spread_done(i):
        pltpu.make_async_copy(whole[i], whole[i], zrecv.at[i]).wait()

    def ring(c, way, step, half):
        block = lax.rem(blk + (nx - step + 1 if way == 0 else step - 1), nx)
        piece = gx.at[c, block, pl.ds(half * part, part), :]
        return pltpu.make_async_remote_copy(
            src_ref=piece,
            dst_ref=piece,
            send_sem=xsend.at[c, way, step - 1, half],
            recv_sem=xrecv.at[c, way, step - 1, half],
            device_id={"blk": right if way == 0 else left},
            device_id_type=MESH,
        )

    def travels(way, step, half):
        return step < hops or (step == hops and way == half)

    def begin(c):
        for half in range(2):
            for way in range(2):
                if travels(way, 1, half):
                    ring(c, way, 1, half).start()

    def advance(c, step):
        for half in range(2):
            for way in range(2):
                if travels(way, step, half):
                    ring(c, way, step, half).wait_recv()
                    if travels(way, step + 1, half):
                        ring(c, way, step + 1, half).start()

    qtile = 256

    def attend(h, block):
        if h == 0:
            vt[block] = gx[1, block].T
        keys = gx[2 * h, block]
        values = vt[block, pl.ds(h * patch, patch), :]
        for t in range(rows // qtile):
            at = pl.ds(t * qtile, qtile)
            scores = lax.dot_general(
                keys, qx[h, at, :], (((1,), (1,)), ((), ())),
                preferred_element_type=jnp.float32,
            )
            old = top[h, :, at]
            new = jnp.maximum(old, jnp.max(scores, axis=0, keepdims=True))
            expo = jnp.exp2(scores * EXP_SCALE - new * EXP_SCALE)
            factor = jnp.exp2((old - new) * EXP_SCALE)
            top[h, :, at] = new
            total[h, :, at] = total[h, :, at] * factor + jnp.sum(expo, axis=0, keepdims=True)
            acc[h, :, at] = acc[h, :, at] * factor + jnp.dot(
                values, expo.astype(jnp.bfloat16), preferred_element_type=jnp.float32
            )

    def near(h, step):
        def one(way, _):
            block = lax.rem(blk + jnp.where(way == 0, nx - step, step), nx)
            attend(h, block)
            return 0

        lax.fori_loop(0, 2, one, 0)

    for i in range(5):
        spread(i)
    top[...] = jnp.full(top.shape, -1e30, jnp.float32)
    total[...] = jnp.zeros(total.shape, jnp.float32)
    acc[...] = jnp.zeros(acc.shape, jnp.float32)

    spread_done(0)
    begin(0)
    for step in range(1, hops - 1):
        advance(0, step)
    spread_done(1)
    begin(1)
    for step in range(hops - 1, hops + 1):
        advance(0, step)
    spread_done(2)
    attend(0, blk)
    for step in range(1, hops):
        advance(1, step)
        if step == hops - 1:
            spread_done(3)
            begin(2)
        near(0, step)
    advance(1, hops)
    attend(0, lax.rem(blk + hops, nx))
    spread_done(4)
    attend(1, blk)
    for step in range(1, hops):
        advance(2, step)
        near(1, step)
    advance(2, hops)
    attend(1, lax.rem(blk + hops, nx))

    velocity = acc[0] / total[0] + acc[1] / total[1]
    wide = jnp.concatenate([velocity, jnp.zeros_like(velocity)], axis=0)
    out_ref[...] = wide.T.astype(jnp.bfloat16)

    for i in range(5):
        sent = whole[i].at[pl.ds(0, rows - tok), :]
        pltpu.make_async_copy(sent, sent, zsend.at[i]).wait()
    for c in range(3):
        for step in range(1, hops + 1):
            for half in range(2):
                for way in range(2):
                    if travels(way, step, half):
                        ring(c, way, step, half).wait_send()


def share_of_velocity(queries, key_states, value_states, head_weight):
    nz = lax.axis_size("seq")
    nx = lax.axis_size("blk")
    tok = queries.shape[0]
    rows = nz * tok
    patch = head_weight.shape[1]
    vmem = pl.BlockSpec(memory_space=pltpu.VMEM)
    return pl.pallas_call(
        functools.partial(exchange_kernel, nz, nx),
        out_shape=jax.ShapeDtypeStruct((rows, 2 * patch), jnp.bfloat16),
        in_specs=[vmem] * 4,
        out_specs=vmem,
        scratch_shapes=[
            pltpu.VMEM((nz, tok, 2 * patch), jnp.bfloat16),
            pltpu.VMEM((3, nx, rows, HDIM), jnp.bfloat16),
            pltpu.VMEM((2, rows, HDIM), jnp.bfloat16),
            pltpu.VMEM((nx, 2 * patch, rows), jnp.bfloat16),
            pltpu.VMEM((2, 1, rows), jnp.float32),
            pltpu.VMEM((2, 1, rows), jnp.float32),
            pltpu.VMEM((2, patch, rows), jnp.float32),
            pltpu.SemaphoreType.DMA((5,)),
            pltpu.SemaphoreType.DMA((5,)),
            pltpu.SemaphoreType.DMA((3, 2, nx // 2, 2)),
            pltpu.SemaphoreType.DMA((3, 2, nx // 2, 2)),
        ],
        compiler_params=pltpu.CompilerParams(collective_id=0, has_side_effects=True),
    )(queries, key_states, value_states, head_weight)


def split_up(array, dim, devices):
    lengths = array.shape
    pieces = array.reshape(*lengths[:dim], devices, lengths[dim] // devices, *lengths[dim + 1 :])
    return jnp.moveaxis(pieces, dim, 0)


def sum_at_owner(array, axis, dim):
    devices = lax.axis_size(axis)
    pieces = lax.all_to_all(split_up(array, dim, devices), axis, 0, 0, tiled=True)
    return jnp.sum(pieces.astype(jnp.float32), axis=0)


def partner(array, axis, apart):
    return lax.ppermute(array, axis, [(i, i ^ 1 << apart) for i in range(lax.axis_size(axis))])


def padded(array, sides, width):
    for axis, dim in sides:
        devices, length = (lax.axis_size(axis), array.shape[dim])
        up = [(i, (i + 1) % devices) for i in range(devices - 1)]
        down = [(j, i) for i, j in up]
        last = lax.slice_in_dim(array, length - width, length, axis=dim)
        first = lax.slice_in_dim(array, 0, width, axis=dim)
        before = lax.ppermute(last, axis, up)
        after = lax.ppermute(first, axis, down)
        array = jnp.concatenate([before, array, after], axis=dim)
    return array


def local(
    queries,
    key_states,
    value_states,
    noisy_latents,
    patch_order,
    head_weight,
    latent_std,
    latent_mean,
    conv_weight,
    conv_bias,
):
    seq_count = lax.axis_size("seq")
    blk_count = lax.axis_size("blk")
    seq_index = lax.axis_index("seq")
    blk_index = lax.axis_index("blk")
    cfg_index = lax.axis_index("cfg")
    tok_rows = queries.shape[1]
    share = share_of_velocity(queries[0], key_states[0], value_states[0], head_weight)
    velocity = sum_at_owner(share[:, : head_weight.shape[1]], "seq", 0)
    other = partner(velocity, "cfg", 0)
    is_cond = cfg_index == 0
    cond = jnp.where(is_cond, velocity, other)
    uncond = jnp.where(is_cond, other, velocity)
    guided = uncond + GUIDE * (cond - uncond)
    denoised = noisy_latents - NOISE_LEVEL * guided
    pixels = (
        denoised * jnp.tile(latent_std, 4)[None, :] + jnp.tile(latent_mean, 4)[None, :]
    ).astype(jnp.bfloat16)
    block_start = (blk_index * seq_count + seq_index) * tok_rows
    local_slot = patch_order - block_start
    selector = (jnp.arange(tok_rows, dtype=jnp.int32)[:, None] == local_slot[None, :]).astype(
        jnp.bfloat16
    )
    placed = jnp.dot(selector, pixels, preferred_element_type=jnp.float32).astype(jnp.bfloat16)
    grid_cols = COLS_DEV * blk_count
    strip_rows = tok_rows // grid_cols
    strip = placed.reshape(1, strip_rows, grid_cols * placed.shape[1])
    received = lax.all_to_all(strip, "blk", split_axis=2, concat_axis=0, tiled=True)
    frame_count = received.shape[0]
    tile = (
        received.reshape(frame_count, strip_rows, COLS_DEV, 2, 2, ZCH)
        .transpose(0, 1, 3, 2, 4, 5)
        .reshape(frame_count, 2 * strip_rows, 2 * COLS_DEV, ZCH)
    )
    half = frame_count // 2
    leading = jnp.zeros((2,) + tile.shape[1:], jnp.bfloat16)
    timeline = jnp.concatenate([leading, tile], axis=0)
    window = lax.dynamic_slice_in_dim(timeline, cfg_index * half, half + 2, 0)
    framed = padded(window, (("seq", 1), ("blk", 2)), 1)
    tile_rows = 2 * strip_rows
    tile_cols = 2 * COLS_DEV
    columns = []
    for step_t in range(3):
        for step_y in range(3):
            for step_x in range(3):
                columns.append(
                    framed[
                        step_t : step_t + half,
                        step_y : step_y + tile_rows,
                        step_x : step_x + tile_cols,
                        :,
                    ]
                )
    stacked = jnp.concatenate(columns, axis=3).reshape(half * tile_rows * tile_cols, 27 * ZCH)
    kernel = conv_weight.reshape(27 * ZCH, conv_weight.shape[4])
    output = jnp.dot(stacked, kernel, preferred_element_type=jnp.float32) + conv_bias[None, :]
    return output.reshape(half, tile_rows, tile_cols, conv_weight.shape[4]).astype(jnp.bfloat16)


def solution(mesh):
    in_specs = (
        P("cfg", ("prompt", "blk", "seq"), None),
        P("cfg", ("prompt", "blk", "seq"), None),
        P("cfg", ("prompt", "blk", "seq"), None),
        P(("prompt", "blk", "seq"), None),
        P(("prompt", "blk", "seq")),
        P(),
        P(),
        P(),
        P(),
        P(),
    )
    out_specs = P(("prompt", "cfg"), "seq", "blk", None)
    return jax.shard_map(local, mesh=mesh, in_specs=in_specs, out_specs=out_specs, check_vma=False)
```

```python
import functools
import math

import jax
import jax.numpy as jnp
from jax import lax
from jax.experimental import pallas as pl
from jax.experimental.pallas import tpu as pltpu
from jax.sharding import PartitionSpec as P

HDIM = 128
ZCH = 16
COLS_DEV = 3
ROW_PAD = 8
TAP_LANES = 256
GUIDE = 5.0
NOISE_LEVEL = 0.5
MESH = pl.DeviceIdType.MESH
EXP_SCALE = math.log2(math.e) / math.sqrt(HDIM)


def exchange_kernel(
    nz, nx, q_ref, k_ref, v_ref, w_ref, noisy_ref, order_ref, std_ref, mean_ref, taps_ref, bias_ref, out_ref,
    vsend, gx, qx, vt, top, total, acc, wide, vout, vin, psend, tile, halo, grid, xcol, wexp, final,
    zsend, zrecv, xsend, xrecv, vsent, vrecv, psent, precv,
):
    seq = lax.axis_index("seq")
    blk = lax.axis_index("blk")
    cfg = lax.axis_index("cfg")
    tok = q_ref.shape[0]
    rows = gx.shape[2]
    part = rows // 2
    patch = w_ref.shape[0]
    frames = nx // 2
    few = tok // 2
    hops = nx // 2
    right = lax.rem(blk + 1, nx)
    left = lax.rem(blk + nx - 1, nx)

    barrier = pltpu.get_barrier_semaphore()

    def greet(s, b):
        for c in range(2):
            pl.semaphore_signal(
                barrier, inc=1, device_id={"seq": s, "blk": b, "cfg": c}, device_id_type=MESH
            )

    def greet_seq(d, _):
        greet(lax.rem(seq + d, nz), blk)
        return 0

    def greet_blk(d, _):
        b = lax.rem(blk + d, nx)
        for near in (0, 1, nz - 1):
            greet(lax.rem(seq + near, nz), b)
        return 0

    xcol[...] = jnp.zeros(xcol.shape, jnp.float32)
    lax.fori_loop(1, nz, greet_seq, 0)
    lax.fori_loop(1, nx, greet_blk, 0)
    pl.semaphore_signal(barrier, inc=1, device_id={"cfg": 1 - cfg}, device_id_type=MESH)

    def project(s, _):
        both = []
        for h in range(2):
            at = pl.ds(pl.multiple_of((2 * s + h) * HDIM, HDIM), HDIM)
            both.append(
                lax.dot_general(
                    v_ref[:, at], w_ref[:, at], (((1,), (1,)), ((), ())),
                    preferred_element_type=jnp.float32,
                )
            )
        vsend[s] = jnp.concatenate(both, axis=1).astype(jnp.bfloat16)
        return 0

    lax.fori_loop(0, nz, project, 0)
    wexp[...] = jnp.zeros(wexp.shape, jnp.bfloat16)
    for step_t in range(3):
        for step_y in range(3):
            taps = taps_ref[pl.ds((3 * step_t + step_y) * 3 * ZCH, 3 * ZCH), :]
            at = step_t * TAP_LANES + step_y * 4 * ZCH
            wexp[0, pl.ds(at + ZCH, 3 * ZCH), :] = taps
            wexp[1, pl.ds(at, 3 * ZCH), :] = taps
    pl.semaphore_wait(barrier, 2 * (nz - 1) + 6 * (nx - 1) + 1)

    own_rows = pl.ds(pl.multiple_of(seq * tok, tok), tok)

    def columns(ref, s, h):
        return ref.at[:, pl.ds(pl.multiple_of((2 * s + h) * HDIM, HDIM), HDIM)]

    sources = (
        lambda s: columns(k_ref, s, 0),
        lambda s: vsend.at[s],
        lambda s: columns(q_ref, s, 0),
        lambda s: columns(k_ref, s, 1),
        lambda s: columns(q_ref, s, 1),
    )
    whole = (gx.at[0, blk], gx.at[1, blk], qx.at[0], gx.at[2, blk], qx.at[1])

    def spread(i):
        pltpu.make_async_copy(
            sources[i](seq), whole[i].at[own_rows, :], zrecv.at[i]
        ).start()

        def send(d, _):
            far = (d + 1) // 2
            peer = lax.rem(seq + jnp.where(lax.rem(d, 2) == 1, far, nz - far), nz)
            pltpu.make_async_remote_copy(
                src_ref=sources[i](peer),
                dst_ref=whole[i].at[own_rows, :],
                send_sem=zsend.at[i],
                recv_sem=zrecv.at[i],
                device_id={"seq": peer},
                device_id_type=MESH,
            ).start()
            return 0

        lax.fori_loop(1, nz, send, 0)

    def spread_done(i):
        pltpu.make_async_copy(whole[i], whole[i], zrecv.at[i]).wait()

    def ring(c, way, step, half):
        block = lax.rem(blk + (nx - step + 1 if way == 0 else step - 1), nx)
        piece = gx.at[c, block, pl.ds(half * part, part), :]
        return pltpu.make_async_remote_copy(
            src_ref=piece,
            dst_ref=piece,
            send_sem=xsend.at[c, way, step - 1, half],
            recv_sem=xrecv.at[c, way, step - 1, half],
            device_id={"blk": right if way == 0 else left},
            device_id_type=MESH,
        )

    def travels(way, step, half):
        return step < hops or (step == hops and way == half)

    def begin(c):
        for half in range(2):
            for way in range(2):
                if travels(way, 1, half):
                    ring(c, way, 1, half).start()

    def advance(c, step):
        for half in range(2):
            for way in range(2):
                if travels(way, step, half):
                    ring(c, way, step, half).wait_recv()
                    if travels(way, step + 1, half):
                        ring(c, way, step + 1, half).start()

    qtile = 256

    def attend(h, block):
        if h == 0:
            vt[block] = gx[1, block].T
        keys = gx[2 * h, block]
        values = vt[block, pl.ds(h * patch, patch), :]
        for t in range(rows // qtile):
            at = pl.ds(t * qtile, qtile)
            scores = lax.dot_general(
                keys, qx[h, at, :], (((1,), (1,)), ((), ())),
                preferred_element_type=jnp.float32,
            )
            old = top[h, :, at]
            new = jnp.maximum(old, jnp.max(scores, axis=0, keepdims=True))
            expo = jnp.exp2(scores * EXP_SCALE - new * EXP_SCALE)
            factor = jnp.exp2((old - new) * EXP_SCALE)
            top[h, :, at] = new
            total[h, :, at] = total[h, :, at] * factor + jnp.sum(expo, axis=0, keepdims=True)
            acc[h, :, at] = acc[h, :, at] * factor + jnp.dot(
                values, expo.astype(jnp.bfloat16), preferred_element_type=jnp.float32
            )

    def near(h, step):
        def one(way, _):
            block = lax.rem(blk + jnp.where(way == 0, nx - step, step), nx)
            attend(h, block)
            return 0

        lax.fori_loop(0, 2, one, 0)

    for i in range(5):
        spread(i)
    top[...] = jnp.full(top.shape, -1e30, jnp.float32)
    total[...] = jnp.zeros(total.shape, jnp.float32)
    acc[...] = jnp.zeros(acc.shape, jnp.float32)

    spread_done(0)
    begin(0)
    for step in range(1, hops - 1):
        advance(0, step)
    spread_done(1)
    begin(1)
    for step in range(hops - 1, hops + 1):
        advance(0, step)
    spread_done(2)
    attend(0, blk)
    for step in range(1, hops):
        advance(1, step)
        if step == hops - 1:
            spread_done(3)
            begin(2)
        near(0, step)
    advance(1, hops)
    attend(0, lax.rem(blk + hops, nx))
    spread_done(4)
    attend(1, blk)
    for step in range(1, hops):
        advance(2, step)
        near(1, step)
    advance(2, hops)
    attend(1, lax.rem(blk + hops, nx))

    velocity = acc[0] / total[0] + acc[1] / total[1]
    velocity = velocity * jnp.where(cfg == 0, GUIDE, 1.0 - GUIDE)
    later = pltpu.roll(velocity, rows - few, 1)
    wide[...] = jnp.concatenate([velocity, later], axis=0).T

    def pack(s, _):
        vout[s] = wide[pl.ds(pl.multiple_of(s * tok, 16), few), :].astype(jnp.bfloat16)
        return 0

    lax.fori_loop(0, nz, pack, 0)
    slot = cfg * nz + seq

    def share(peer):
        return pltpu.make_async_remote_copy(
            src_ref=vout.at[peer],
            dst_ref=vin.at[slot],
            send_sem=vsent,
            recv_sem=vrecv,
            device_id={"seq": peer, "cfg": 1},
            device_id_type=MESH,
        )

    def send_share(d, _):
        far = nz // 2 - d // 2
        share(lax.rem(seq + jnp.where(lax.rem(d, 2) == 1, far, nz - far), nz)).start()
        return 0

    lax.fori_loop(1, nz, send_share, 0)

    @pl.when(cfg == 0)
    def _():
        share(seq).start()
        pltpu.make_async_copy(vout, vout, vsent).wait()

    def greater(target_cfg):
        return blk < frames if target_cfg == 0 else blk >= frames - 2

    @pl.when(cfg == 1)
    def _():
        pltpu.make_async_copy(vout.at[seq], vin.at[slot], vrecv).start()
        pltpu.make_async_copy(vin, vin, vrecv).wait()
        guided = jnp.sum(vin[...].astype(jnp.float32), axis=0)
        noisy = jnp.concatenate([noisy_ref[0:few, :], noisy_ref[few:tok, :]], axis=1)
        scale = jnp.concatenate([std_ref[...]] * (2 * patch // ZCH), axis=1)
        shift = jnp.concatenate([mean_ref[...]] * (2 * patch // ZCH), axis=1)
        pixels = (noisy - NOISE_LEVEL * guided) * scale + shift
        pixels = jnp.concatenate([pixels[:, :patch], pixels[:, patch:]], axis=0).astype(jnp.bfloat16)

        entry = lax.broadcasted_iota(jnp.int32, (patch, 2 * patch), 0)
        lane = lax.broadcasted_iota(jnp.int32, (patch, 2 * patch), 1)
        half = patch // 2
        spread_pixels = []
        for p in range(2):
            place = (
                (entry // half == lane // patch)
                & (entry % half == lane % half)
                & ((lane // half) % 2 == p)
            ).astype(jnp.bfloat16)
            spread_pixels.append(jnp.dot(pixels, place, preferred_element_type=jnp.float32))
        spread_pixels = jnp.concatenate(spread_pixels, axis=0).astype(jnp.bfloat16)
        slots = order_ref[...] - (blk * nz + seq) * tok
        slots = jnp.concatenate([slots, slots], axis=1)
        row = lax.broadcasted_iota(jnp.int32, (ROW_PAD * nx, 2 * tok), 0)
        token = lax.broadcasted_iota(jnp.int32, (ROW_PAD * nx, 2 * tok), 1)
        x = row % ROW_PAD
        column = COLS_DEV * (row // ROW_PAD) - 1 + (x + 1) // 2 + token // tok
        inside = (x < 2 * COLS_DEV) & (column >= 0) & (column < COLS_DEV * nx)
        for i in range(2):
            select = (inside & (slots == column + i * COLS_DEV * nx)).astype(jnp.bfloat16)
            picked = jnp.dot(select, spread_pixels, preferred_element_type=jnp.float32)
            psend[:, :, i * 2 * patch : (i + 1) * 2 * patch] = picked.reshape(
                nx, ROW_PAD, 2 * patch
            ).astype(jnp.bfloat16)

        above = lax.rem(seq + nz - 1, nz)
        below = lax.rem(seq + 1, nz)
        pieces = (
            (0, pl.ds(0, 4 * patch), tile.at[blk], seq),
            (1, pl.ds(2 * patch, 2 * patch), halo.at[blk, 0], below),
            (1, pl.ds(0, 2 * patch), halo.at[blk, 1], above),
        )
        for c in range(2):

            @pl.when(greater(c))
            def _():
                def send_pieces(d, _):
                    b = lax.rem(blk + d, nx)
                    for kind, at, there, s in pieces:
                        pltpu.make_async_remote_copy(
                            src_ref=psend.at[b, :, at],
                            dst_ref=there,
                            send_sem=psent.at[c, kind],
                            recv_sem=precv.at[kind],
                            device_id={"seq": s, "blk": b, "cfg": c},
                            device_id_type=MESH,
                        ).start()
                    return 0

                lax.fori_loop(1, nx, send_pieces, 0)
                for kind, at, there, s in pieces:
                    if c == 1 and kind == 0:
                        pltpu.make_async_copy(psend.at[blk, :, at], there, precv.at[0]).start()
                    else:
                        pltpu.make_async_remote_copy(
                            src_ref=psend.at[blk, :, at],
                            dst_ref=there,
                            send_sem=psent.at[c, kind],
                            recv_sem=precv.at[kind],
                            device_id={"seq": s, "cfg": c},
                            device_id_type=MESH,
                        ).start()

    for c in range(2):

        @pl.when(cfg == c)
        def _():
            arrived = pl.ds(0, frames) if c == 0 else pl.ds(frames - 2, frames + 2)
            pltpu.make_async_copy(tile.at[arrived], tile.at[arrived], precv.at[0]).wait()
            pltpu.make_async_copy(halo.at[arrived], halo.at[arrived], precv.at[1]).wait()

    def line(g, _):
        frame = cfg * frames - 2 + g
        known = frame >= 0
        frame = jnp.maximum(frame, 0)
        upper = halo[frame, 0].astype(jnp.float32)[:, patch:]
        lower = halo[frame, 1].astype(jnp.float32)[:, :patch]
        upper = jnp.where(known & (seq > 0), upper, 0.0)
        lower = jnp.where(known & (seq < nz - 1), lower, 0.0)
        middle = jnp.where(known, tile[frame].astype(jnp.float32), 0.0)
        grid[g] = jnp.concatenate([upper, middle, lower], axis=1)
        return 0

    lax.fori_loop(0, frames + 2, line, 0)
    for f in range(frames):
        for y in range(4):
            for step_t in range(3):
                xcol[pl.ds((4 * f + y) * ROW_PAD, ROW_PAD), pl.ds(step_t * TAP_LANES, 3 * patch)] = grid[
                    f + step_t, :, pl.ds(y * patch, 3 * patch)
                ]
    odd = lax.broadcasted_iota(jnp.int32, xcol.shape, 0) % 2 == 1
    features = bias_ref[...]
    for parity in range(2):
        kept = jnp.where(odd if parity else ~odd, xcol[...], 0.0).astype(jnp.bfloat16)
        features = features + jnp.dot(kept, wexp[parity], preferred_element_type=jnp.float32)
    wide_x = 2 * COLS_DEV
    to = lax.broadcasted_iota(jnp.int32, (frames * wide_x * 4, xcol.shape[0]), 0)
    at = lax.broadcasted_iota(jnp.int32, (frames * wide_x * 4, xcol.shape[0]), 1)
    source = ((to // (4 * wide_x)) * 4 + to % 4) * ROW_PAD + (to // 4) % wide_x
    order = (source == at).astype(jnp.bfloat16)
    final[...] = jnp.dot(order, features.astype(jnp.bfloat16), preferred_element_type=jnp.float32)
    for f in range(frames):
        for x in range(wide_x):
            out_ref[f, x] = final[pl.ds((f * wide_x + x) * 4, 4), :].astype(jnp.bfloat16)

    @pl.when(cfg == 1)
    def _():
        sent = vout.at[pl.ds(0, nz - 1)]
        pltpu.make_async_copy(sent, sent, vsent).wait()
        for c in range(2):

            @pl.when(greater(c))
            def _():
                tiles = psend.at[pl.ds(0, nx - c)]
                pltpu.make_async_copy(tiles, tiles, psent.at[c, 0]).wait()
                pltpu.make_async_copy(psend, psend, psent.at[c, 1]).wait()

    for i in range(5):
        sent = whole[i].at[pl.ds(0, rows - tok), :]
        pltpu.make_async_copy(sent, sent, zsend.at[i]).wait()
    for c in range(3):
        for step in range(1, hops + 1):
            for half in range(2):
                for way in range(2):
                    if travels(way, step, half):
                        ring(c, way, step, half).wait_send()


def local(
    queries,
    key_states,
    value_states,
    noisy_latents,
    patch_order,
    head_weight,
    latent_std,
    latent_mean,
    conv_weight,
    conv_bias,
):
    nz = lax.axis_size("seq")
    nx = lax.axis_size("blk")
    tok = queries.shape[1]
    rows = nz * tok
    patch = head_weight.shape[1]
    wide = conv_weight.shape[4]
    frames = nx // 2
    pixels = 4 * frames * ROW_PAD
    vmem = pl.BlockSpec(memory_space=pltpu.VMEM)
    features = pl.pallas_call(
        functools.partial(exchange_kernel, nz, nx),
        out_shape=jax.ShapeDtypeStruct((frames, 2 * COLS_DEV, 4, wide), jnp.bfloat16),
        in_specs=[vmem] * 10,
        out_specs=vmem,
        scratch_shapes=[
            pltpu.VMEM((nz, tok, 2 * patch), jnp.bfloat16),
            pltpu.VMEM((3, nx, rows, HDIM), jnp.bfloat16),
            pltpu.VMEM((2, rows, HDIM), jnp.bfloat16),
            pltpu.VMEM((nx, 2 * patch, rows), jnp.bfloat16),
            pltpu.VMEM((2, 1, rows), jnp.float32),
            pltpu.VMEM((2, 1, rows), jnp.float32),
            pltpu.VMEM((2, patch, rows), jnp.float32),
            pltpu.VMEM((rows, 2 * patch), jnp.float32),
            pltpu.VMEM((nz, tok // 2, 2 * patch), jnp.bfloat16),
            pltpu.VMEM((2 * nz, tok // 2, 2 * patch), jnp.bfloat16),
            pltpu.VMEM((nx, ROW_PAD, 4 * patch), jnp.bfloat16),
            pltpu.VMEM((nx, ROW_PAD, 4 * patch), jnp.bfloat16),
            pltpu.VMEM((nx, 2, ROW_PAD, 2 * patch), jnp.bfloat16),
            pltpu.VMEM((frames + 2, ROW_PAD, 6 * patch), jnp.float32),
            pltpu.VMEM((pixels, 3 * TAP_LANES), jnp.float32),
            pltpu.VMEM((2, 3 * TAP_LANES, wide), jnp.bfloat16),
            pltpu.VMEM((8 * frames * COLS_DEV, wide), jnp.float32),
            pltpu.SemaphoreType.DMA((5,)),
            pltpu.SemaphoreType.DMA((5,)),
            pltpu.SemaphoreType.DMA((3, 2, nx // 2, 2)),
            pltpu.SemaphoreType.DMA((3, 2, nx // 2, 2)),
            pltpu.SemaphoreType.DMA,
            pltpu.SemaphoreType.DMA,
            pltpu.SemaphoreType.DMA((2, 2)),
            pltpu.SemaphoreType.DMA((2,)),
        ],
        compiler_params=pltpu.CompilerParams(collective_id=0, has_side_effects=True),
    )(
        queries[0],
        key_states[0],
        value_states[0],
        head_weight.T,
        noisy_latents,
        patch_order.reshape(1, tok),
        latent_std.reshape(1, ZCH),
        latent_mean.reshape(1, ZCH),
        conv_weight.reshape(27 * ZCH, wide),
        conv_bias.reshape(1, wide),
    )
    return features.transpose(0, 2, 1, 3)


def solution(mesh):
    in_specs = (
        P("cfg", ("prompt", "blk", "seq"), None),
        P("cfg", ("prompt", "blk", "seq"), None),
        P("cfg", ("prompt", "blk", "seq"), None),
        P(("prompt", "blk", "seq"), None),
        P(("prompt", "blk", "seq")),
        P(),
        P(),
        P(),
        P(),
        P(),
    )
    out_specs = P(("prompt", "cfg"), "seq", "blk", None)
    return jax.shard_map(local, mesh=mesh, in_specs=in_specs, out_specs=out_specs, check_vma=False)
```

```python
import functools
import math

import jax
import jax.numpy as jnp
from jax import lax
from jax.experimental import pallas as pl
from jax.experimental.pallas import tpu as pltpu
from jax.sharding import PartitionSpec as P

HDIM = 128
ZCH = 16
COLS_DEV = 3
ROW_PAD = 8
TAP_LANES = 256
ONES = 16
GUIDE = 5.0
NOISE_LEVEL = 0.5
MESH = pl.DeviceIdType.MESH
EXP_SCALE = math.log2(math.e) / math.sqrt(HDIM)


def exchange_kernel(
    nz, nx, q_ref, k_ref, v_ref, w_ref, noisy_ref, order_ref, std_ref, mean_ref, taps_ref, bias_ref, out_ref,
    vsend, gx, qx, vt, top, acc, wide, vout, vin, psend, tile, halo, grid, xcol, wexp, final,
    zsend, zrecv, xsend, xrecv, vsent, vrecv, psent, precv,
):
    seq = lax.axis_index("seq")
    blk = lax.axis_index("blk")
    cfg = lax.axis_index("cfg")
    tok = q_ref.shape[0]
    rows = gx.shape[2]
    part = rows // 2
    patch = w_ref.shape[0]
    frames = nx // 2
    few = tok // 2
    hops = nx // 2
    right = lax.rem(blk + 1, nx)
    left = lax.rem(blk + nx - 1, nx)

    barrier = pltpu.get_barrier_semaphore()

    def greet(s, b):
        for c in range(2):
            pl.semaphore_signal(
                barrier, inc=1, device_id={"seq": s, "blk": b, "cfg": c}, device_id_type=MESH
            )

    def greet_seq(d, _):
        greet(lax.rem(seq + d, nz), blk)
        return 0

    def greet_blk(d, _):
        b = lax.rem(blk + d, nx)
        for near in (0, 1, nz - 1):
            greet(lax.rem(seq + near, nz), b)
        return 0

    lax.fori_loop(1, nz, greet_seq, 0)
    lax.fori_loop(1, nx, greet_blk, 0)
    pl.semaphore_signal(barrier, inc=1, device_id={"cfg": 1 - cfg}, device_id_type=MESH)

    pl.semaphore_wait(barrier, 2 * (nz - 1) + 6 * (nx - 1) + 1)

    def project(s, _):
        both = []
        for h in range(2):
            at = pl.ds(pl.multiple_of((2 * s + h) * HDIM, HDIM), HDIM)
            both.append(
                lax.dot_general(
                    v_ref[:, at], w_ref[:, at], (((1,), (1,)), ((), ())),
                    preferred_element_type=jnp.float32,
                )
            )
        vsend[s] = jnp.concatenate(both, axis=1).astype(jnp.bfloat16)
        return 0

    def columns(ref, first, count, s, h):
        return ref.at[pl.ds(first, count), pl.ds(pl.multiple_of((2 * s + h) * HDIM, HDIM), HDIM)]

    def half_of(c, half):
        there = gx.at[c, blk, pl.ds(half * part, part), :]
        if c == 1:
            return lambda s: vsend.at[s, pl.ds(half * few, few), :], there, few
        return lambda s: columns(k_ref, half * few, few, s, c // 2), there, few

    def query_of(h):
        return lambda s: columns(q_ref, 0, tok, s, h), qx.at[h], tok

    parcels = (
        half_of(0, 0), half_of(0, 1), half_of(1, 0), half_of(1, 1), query_of(0),
        half_of(2, 0), half_of(2, 1), query_of(1),
    )

    def spread(i):
        source, whole, count = parcels[i]
        there = whole.at[pl.ds(pl.multiple_of(seq * count, 8), count), :]
        pltpu.make_async_copy(source(seq), there, zrecv.at[i]).start()

        def send(d, _):
            far = nz // 2 - d // 2
            peer = lax.rem(seq + jnp.where(lax.rem(d, 2) == 1, far, nz - far), nz)
            pltpu.make_async_remote_copy(
                src_ref=source(peer),
                dst_ref=there,
                send_sem=zsend.at[i],
                recv_sem=zrecv.at[i],
                device_id={"seq": peer},
                device_id_type=MESH,
            ).start()
            return 0

        lax.fori_loop(1, nz, send, 0)

    def spread_done(i):
        whole = parcels[i][1]
        pltpu.make_async_copy(whole, whole, zrecv.at[i]).wait()

    def ring(c, way, step, half):
        block = lax.rem(blk + (nx - step + 1 if way == 0 else step - 1), nx)
        piece = gx.at[c, block, pl.ds(half * part, part), :]
        return pltpu.make_async_remote_copy(
            src_ref=piece,
            dst_ref=piece,
            send_sem=xsend.at[c, way, step - 1, half],
            recv_sem=xrecv.at[c, way, step - 1, half],
            device_id={"blk": right if way == 0 else left},
            device_id_type=MESH,
        )

    def travels(way, step, half):
        return step < hops or (step == hops and way == half)

    def begin(c, half):
        for way in range(2):
            if travels(way, 1, half):
                ring(c, way, 1, half).start()

    def advance(c, step, half, way):
        if travels(way, step, half):
            ring(c, way, step, half).wait_recv()
            if travels(way, step + 1, half):
                ring(c, way, step + 1, half).start()

    def advance_all(c, step):
        for half in range(2):
            for way in range(2):
                advance(c, step, half, way)

    qtile = rows // 2

    def attend(h, blocks):
        if h == 0:
            for block in blocks:
                turned = gx[1, block].T
                for g in range(2):
                    vt[block, g, pl.ds(0, patch), :] = turned[g * patch : (g + 1) * patch, :]
        items = [(block, t) for block in blocks for t in range(rows // qtile)]

        def scores_of(block, t):
            return lax.dot_general(
                gx[2 * h, block], qx[h, pl.ds(t * qtile, qtile), :], (((1,), (1,)), ((), ())),
                preferred_element_type=jnp.float32,
            )

        ahead = len(blocks)
        ready = [scores_of(*item) for item in items[:ahead]]
        for n, (block, t) in enumerate(items):
            if n + ahead < len(items):
                ready.append(scores_of(*items[n + ahead]))
            scores = ready.pop(0)
            at = pl.ds(t * qtile, qtile)
            old = top[h, :, at]
            new = jnp.maximum(old, jnp.max(scores, axis=0, keepdims=True))
            expo = jnp.exp2(scores * EXP_SCALE - new * EXP_SCALE).astype(jnp.bfloat16)
            factor = jnp.exp2((old - new) * EXP_SCALE)
            top[h, :, at] = new
            acc[h, :, at] = acc[h, :, at] * factor + jnp.dot(
                vt[block, h], expo, preferred_element_type=jnp.float32
            )

    def behind(step):
        return lax.rem(blk + nx - step, nx)

    def beyond(step):
        return lax.rem(blk + step, nx)

    spread(0)
    spread(1)
    lax.fori_loop(0, nz, project, 0)
    for i in range(2, len(parcels)):
        spread(i)
    top[...] = jnp.full(top.shape, -1e30, jnp.float32)
    acc[...] = jnp.zeros(acc.shape, jnp.float32)
    vt[:, :, pl.ds(patch, vt.shape[2] - patch), :] = jnp.ones(
        (nx, 2, vt.shape[2] - patch, rows), jnp.bfloat16
    )
    xcol[...] = jnp.zeros(xcol.shape, jnp.float32)
    wexp[...] = jnp.zeros(wexp.shape, jnp.bfloat16)
    for step_t in range(3):
        for step_y in range(3):
            taps = taps_ref[pl.ds((3 * step_t + step_y) * 3 * ZCH, 3 * ZCH), :]
            at = step_t * TAP_LANES + step_y * 4 * ZCH
            wexp[0, pl.ds(at + ZCH, 3 * ZCH), :] = taps
            wexp[1, pl.ds(at, 3 * ZCH), :] = taps

    spread_done(0)
    begin(0, 0)
    spread_done(1)
    begin(0, 1)
    advance_all(0, 1)
    spread_done(2)
    begin(1, 0)
    advance_all(0, 2)
    spread_done(3)
    begin(1, 1)
    for step in range(3, hops):
        advance_all(0, step)
    advance_all(1, 1)
    advance_all(0, hops)
    spread_done(4)
    attend(0, [blk])
    for step in range(1, hops):
        if step > 1:
            advance_all(1, step)
        attend(0, [behind(step), beyond(step)])
        if step == 1:
            spread_done(5)
            begin(2, 0)
        if step == 2:
            spread_done(6)
            begin(2, 1)
    advance_all(1, hops)
    advance_all(2, 1)
    attend(0, [beyond(hops)])
    spread_done(7)
    attend(1, [blk])
    for step in range(1, hops):
        if step > 1:
            advance_all(2, step)
        attend(1, [behind(step), beyond(step)])
    advance_all(2, hops)
    attend(1, [beyond(hops)])

    velocity = 0.0
    for h in range(2):
        velocity = velocity + acc[h, pl.ds(0, patch), :] / acc[h, pl.ds(patch, 1), :]
    velocity = velocity * jnp.where(cfg == 0, GUIDE, 1.0 - GUIDE)
    later = pltpu.roll(velocity, rows - few, 1)
    wide[...] = jnp.concatenate([velocity, later], axis=0).T

    def pack(s, _):
        vout[s] = wide[pl.ds(pl.multiple_of(s * tok, 16), few), :].astype(jnp.bfloat16)
        return 0

    lax.fori_loop(0, nz, pack, 0)
    slot = cfg * nz + seq

    def share(peer):
        return pltpu.make_async_remote_copy(
            src_ref=vout.at[peer],
            dst_ref=vin.at[slot],
            send_sem=vsent,
            recv_sem=vrecv,
            device_id={"seq": peer, "cfg": 1},
            device_id_type=MESH,
        )

    def send_share(d, _):
        far = nz // 2 - d // 2
        share(lax.rem(seq + jnp.where(lax.rem(d, 2) == 1, far, nz - far), nz)).start()
        return 0

    lax.fori_loop(1, nz, send_share, 0)

    @pl.when(cfg == 0)
    def _():
        share(seq).start()
        pltpu.make_async_copy(vout, vout, vsent).wait()

    def greater(target_cfg):
        return blk < frames if target_cfg == 0 else blk >= frames - 2

    @pl.when(cfg == 1)
    def _():
        pltpu.make_async_copy(vout.at[seq], vin.at[slot], vrecv).start()
        pltpu.make_async_copy(vin, vin, vrecv).wait()
        guided = jnp.sum(vin[...].astype(jnp.float32), axis=0)
        noisy = jnp.concatenate([noisy_ref[0:few, :], noisy_ref[few:tok, :]], axis=1)
        scale = jnp.concatenate([std_ref[...]] * (2 * patch // ZCH), axis=1)
        shift = jnp.concatenate([mean_ref[...]] * (2 * patch // ZCH), axis=1)
        pixels = (noisy - NOISE_LEVEL * guided) * scale + shift
        pixels = jnp.concatenate([pixels[:, :patch], pixels[:, patch:]], axis=0).astype(jnp.bfloat16)

        entry = lax.broadcasted_iota(jnp.int32, (patch, 2 * patch), 0)
        lane = lax.broadcasted_iota(jnp.int32, (patch, 2 * patch), 1)
        half = patch // 2
        spread_pixels = []
        for p in range(2):
            place = (
                (entry // half == lane // patch)
                & (entry % half == lane % half)
                & ((lane // half) % 2 == p)
            ).astype(jnp.bfloat16)
            spread_pixels.append(jnp.dot(pixels, place, preferred_element_type=jnp.float32))
        spread_pixels = jnp.concatenate(spread_pixels, axis=0).astype(jnp.bfloat16)
        slots = order_ref[...] - (blk * nz + seq) * tok
        slots = jnp.concatenate([slots, slots], axis=1)
        row = lax.broadcasted_iota(jnp.int32, (ROW_PAD * nx, 2 * tok), 0)
        token = lax.broadcasted_iota(jnp.int32, (ROW_PAD * nx, 2 * tok), 1)
        x = row % ROW_PAD
        column = COLS_DEV * (row // ROW_PAD) - 1 + (x + 1) // 2 + token // tok
        inside = (x < 2 * COLS_DEV) & (column >= 0) & (column < COLS_DEV * nx)
        for i in range(2):
            select = (inside & (slots == column + i * COLS_DEV * nx)).astype(jnp.bfloat16)
            picked = jnp.dot(select, spread_pixels, preferred_element_type=jnp.float32)
            psend[:, :, i * 2 * patch : (i + 1) * 2 * patch] = picked.reshape(
                nx, ROW_PAD, 2 * patch
            ).astype(jnp.bfloat16)

        above = lax.rem(seq + nz - 1, nz)
        below = lax.rem(seq + 1, nz)
        pieces = (
            (0, pl.ds(0, 4 * patch), tile.at[blk], seq),
            (1, pl.ds(2 * patch, 2 * patch), halo.at[blk, 0], below),
            (1, pl.ds(0, 2 * patch), halo.at[blk, 1], above),
        )
        for c in range(2):

            @pl.when(greater(c))
            def _():
                def send_pieces(d, _):
                    b = lax.rem(blk + d, nx)
                    for kind, at, there, s in pieces:
                        pltpu.make_async_remote_copy(
                            src_ref=psend.at[b, :, at],
                            dst_ref=there,
                            send_sem=psent.at[c, kind],
                            recv_sem=precv.at[kind],
                            device_id={"seq": s, "blk": b, "cfg": c},
                            device_id_type=MESH,
                        ).start()
                    return 0

                lax.fori_loop(1, nx, send_pieces, 0)
                for kind, at, there, s in pieces:
                    if c == 1 and kind == 0:
                        pltpu.make_async_copy(psend.at[blk, :, at], there, precv.at[0]).start()
                    else:
                        pltpu.make_async_remote_copy(
                            src_ref=psend.at[blk, :, at],
                            dst_ref=there,
                            send_sem=psent.at[c, kind],
                            recv_sem=precv.at[kind],
                            device_id={"seq": s, "cfg": c},
                            device_id_type=MESH,
                        ).start()

    for c in range(2):

        @pl.when(cfg == c)
        def _():
            arrived = pl.ds(0, frames) if c == 0 else pl.ds(frames - 2, frames + 2)
            pltpu.make_async_copy(tile.at[arrived], tile.at[arrived], precv.at[0]).wait()
            pltpu.make_async_copy(halo.at[arrived], halo.at[arrived], precv.at[1]).wait()

    def line(g, _):
        frame = cfg * frames - 2 + g
        known = frame >= 0
        frame = jnp.maximum(frame, 0)
        upper = halo[frame, 0].astype(jnp.float32)[:, patch:]
        lower = halo[frame, 1].astype(jnp.float32)[:, :patch]
        upper = jnp.where(known & (seq > 0), upper, 0.0)
        lower = jnp.where(known & (seq < nz - 1), lower, 0.0)
        middle = jnp.where(known, tile[frame].astype(jnp.float32), 0.0)
        grid[g] = jnp.concatenate([upper, middle, lower], axis=1)
        return 0

    lax.fori_loop(0, frames + 2, line, 0)
    for f in range(frames):
        for y in range(4):
            for step_t in range(3):
                xcol[pl.ds((4 * f + y) * ROW_PAD, ROW_PAD), pl.ds(step_t * TAP_LANES, 3 * patch)] = grid[
                    f + step_t, :, pl.ds(y * patch, 3 * patch)
                ]
    odd = lax.broadcasted_iota(jnp.int32, xcol.shape, 0) % 2 == 1
    features = bias_ref[...]
    for parity in range(2):
        kept = jnp.where(odd if parity else ~odd, xcol[...], 0.0).astype(jnp.bfloat16)
        features = features + jnp.dot(kept, wexp[parity], preferred_element_type=jnp.float32)
    wide_x = 2 * COLS_DEV
    to = lax.broadcasted_iota(jnp.int32, (frames * wide_x * 4, xcol.shape[0]), 0)
    at = lax.broadcasted_iota(jnp.int32, (frames * wide_x * 4, xcol.shape[0]), 1)
    source = ((to // (4 * wide_x)) * 4 + to % 4) * ROW_PAD + (to // 4) % wide_x
    order = (source == at).astype(jnp.bfloat16)
    final[...] = jnp.dot(order, features.astype(jnp.bfloat16), preferred_element_type=jnp.float32)
    for f in range(frames):
        for x in range(wide_x):
            out_ref[f, x] = final[pl.ds((f * wide_x + x) * 4, 4), :].astype(jnp.bfloat16)

    @pl.when(cfg == 1)
    def _():
        sent = vout.at[pl.ds(0, nz - 1)]
        pltpu.make_async_copy(sent, sent, vsent).wait()
        for c in range(2):

            @pl.when(greater(c))
            def _():
                tiles = psend.at[pl.ds(0, nx - c)]
                pltpu.make_async_copy(tiles, tiles, psent.at[c, 0]).wait()
                pltpu.make_async_copy(psend, psend, psent.at[c, 1]).wait()

    for i, (_, whole, count) in enumerate(parcels):
        sent = whole.at[pl.ds(0, (nz - 1) * count), :]
        pltpu.make_async_copy(sent, sent, zsend.at[i]).wait()
    for c in range(3):
        for step in range(1, hops + 1):
            for half in range(2):
                for way in range(2):
                    if travels(way, step, half):
                        ring(c, way, step, half).wait_send()


def local(
    queries,
    key_states,
    value_states,
    noisy_latents,
    patch_order,
    head_weight,
    latent_std,
    latent_mean,
    conv_weight,
    conv_bias,
):
    nz = lax.axis_size("seq")
    nx = lax.axis_size("blk")
    tok = queries.shape[1]
    rows = nz * tok
    patch = head_weight.shape[1]
    wide = conv_weight.shape[4]
    frames = nx // 2
    pixels = 4 * frames * ROW_PAD
    vmem = pl.BlockSpec(memory_space=pltpu.VMEM)
    features = pl.pallas_call(
        functools.partial(exchange_kernel, nz, nx),
        out_shape=jax.ShapeDtypeStruct((frames, 2 * COLS_DEV, 4, wide), jnp.bfloat16),
        in_specs=[vmem] * 10,
        out_specs=vmem,
        scratch_shapes=[
            pltpu.VMEM((nz, tok, 2 * patch), jnp.bfloat16),
            pltpu.VMEM((3, nx, rows, HDIM), jnp.bfloat16),
            pltpu.VMEM((2, rows, HDIM), jnp.bfloat16),
            pltpu.VMEM((nx, 2, patch + ONES, rows), jnp.bfloat16),
            pltpu.VMEM((2, 1, rows), jnp.float32),
            pltpu.VMEM((2, patch + ONES, rows), jnp.float32),
            pltpu.VMEM((rows, 2 * patch), jnp.float32),
            pltpu.VMEM((nz, tok // 2, 2 * patch), jnp.bfloat16),
            pltpu.VMEM((2 * nz, tok // 2, 2 * patch), jnp.bfloat16),
            pltpu.VMEM((nx, ROW_PAD, 4 * patch), jnp.bfloat16),
            pltpu.VMEM((nx, ROW_PAD, 4 * patch), jnp.bfloat16),
            pltpu.VMEM((nx, 2, ROW_PAD, 2 * patch), jnp.bfloat16),
            pltpu.VMEM((frames + 2, ROW_PAD, 6 * patch), jnp.float32),
            pltpu.VMEM((pixels, 3 * TAP_LANES), jnp.float32),
            pltpu.VMEM((2, 3 * TAP_LANES, wide), jnp.bfloat16),
            pltpu.VMEM((8 * frames * COLS_DEV, wide), jnp.float32),
            pltpu.SemaphoreType.DMA((8,)),
            pltpu.SemaphoreType.DMA((8,)),
            pltpu.SemaphoreType.DMA((3, 2, nx // 2, 2)),
            pltpu.SemaphoreType.DMA((3, 2, nx // 2, 2)),
            pltpu.SemaphoreType.DMA,
            pltpu.SemaphoreType.DMA,
            pltpu.SemaphoreType.DMA((2, 2)),
            pltpu.SemaphoreType.DMA((2,)),
        ],
        compiler_params=pltpu.CompilerParams(collective_id=0, has_side_effects=True),
    )(
        queries[0],
        key_states[0],
        value_states[0],
        head_weight.T,
        noisy_latents,
        patch_order.reshape(1, tok),
        latent_std.reshape(1, ZCH),
        latent_mean.reshape(1, ZCH),
        conv_weight.reshape(27 * ZCH, wide),
        conv_bias.reshape(1, wide),
    )
    return features.transpose(0, 2, 1, 3)


def solution(mesh):
    in_specs = (
        P("cfg", ("prompt", "blk", "seq"), None),
        P("cfg", ("prompt", "blk", "seq"), None),
        P("cfg", ("prompt", "blk", "seq"), None),
        P(("prompt", "blk", "seq"), None),
        P(("prompt", "blk", "seq")),
        P(),
        P(),
        P(),
        P(),
        P(),
    )
    out_specs = P(("prompt", "cfg"), "seq", "blk", None)
    return jax.shard_map(local, mesh=mesh, in_specs=in_specs, out_specs=out_specs, check_vma=False)
```

```python
import functools
import math

import jax
import jax.numpy as jnp
from jax import lax
from jax.experimental import pallas as pl
from jax.experimental.pallas import tpu as pltpu
from jax.sharding import PartitionSpec as P

HDIM = 128
ZCH = 16
COLS_DEV = 3
ROW_PAD = 8
TAP_LANES = 256
ONES = 16
GUIDE = 5.0
NOISE_LEVEL = 0.5
MESH = pl.DeviceIdType.MESH
BEGIN, QUERIES, PASS, ATTEND = range(4)
BOTH = 2
ORDER = (
    (BEGIN, 0, 0), (PASS, 0, 1, 0, BOTH), (BEGIN, 0, 1), (PASS, 0, 2, 0, BOTH), (BEGIN, 1, 0),
    (PASS, 0, 1, 1, BOTH), (PASS, 0, 3, 0, BOTH), (PASS, 1, 1, 0, BOTH), (BEGIN, 1, 1),
    (PASS, 0, 2, 1, BOTH), (PASS, 0, 4, 0, 0), (PASS, 1, 2, 0, BOTH), (PASS, 1, 1, 1, BOTH),
    (PASS, 0, 3, 1, 1), (QUERIES, 0), (ATTEND, 0, 0), (PASS, 0, 3, 1, 0), (PASS, 1, 3, 0, 1),
    (ATTEND, 0, -1), (ATTEND, 0, 1), (BEGIN, 2, 0), (PASS, 1, 3, 0, 0), (PASS, 1, 2, 1, 1),
    (ATTEND, 0, 2), (PASS, 1, 2, 1, 0), (PASS, 0, 4, 1, 1), (ATTEND, 0, -2), (PASS, 2, 1, 0, BOTH),
    (BEGIN, 2, 1), (PASS, 1, 4, 0, 0), (PASS, 1, 3, 1, 1), (ATTEND, 0, 3), (PASS, 1, 3, 1, 0),
    (PASS, 2, 2, 0, 1), (ATTEND, 0, -3), (PASS, 2, 2, 0, 0), (PASS, 2, 1, 1, BOTH),
    (PASS, 1, 4, 1, 1), (ATTEND, 0, 4), (QUERIES, 1), (ATTEND, 1, 0), (PASS, 2, 3, 0, BOTH),
    (ATTEND, 1, -1), (ATTEND, 1, 1), (PASS, 2, 2, 1, BOTH), (ATTEND, 1, -2), (ATTEND, 1, 2),
    (PASS, 2, 4, 0, 0), (PASS, 2, 3, 1, BOTH), (ATTEND, 1, -3), (ATTEND, 1, 3), (PASS, 2, 4, 1, 1),
    (ATTEND, 1, 4),
)
EXP_SCALE = math.log2(math.e) / math.sqrt(HDIM)


def exchange_kernel(
    nz, nx, q_hbm, k_hbm, v_hbm, w_hbm, taps_hbm, noisy_ref, order_ref, std_ref, mean_ref, out_ref,
    q_ref, k_ref, v_ref, w_ref, taps_ref,
    vsend, gx, qx, vt, top, acc, wide, vout, vin, psend, tile, halo, grid, xcol, wexp, final,
    zsend, zrecv, xsend, xrecv, vsent, vrecv, psent, precv, loaded,
):
    seq = lax.axis_index("seq")
    blk = lax.axis_index("blk")
    cfg = lax.axis_index("cfg")
    tok = q_ref.shape[0]
    rows = gx.shape[2]
    part = rows // 2
    patch = w_ref.shape[0]
    frames = nx // 2
    few = tok // 2
    hops = nx // 2
    right = lax.rem(blk + 1, nx)
    left = lax.rem(blk + nx - 1, nx)

    barrier = pltpu.get_barrier_semaphore()

    loads = [
        pltpu.make_async_copy(there, here, loaded.at[n])
        for n, (there, here) in enumerate(
            ((k_hbm, k_ref), (v_hbm, v_ref), (w_hbm, w_ref), (q_hbm, q_ref), (taps_hbm, taps_ref))
        )
    ]
    for load in loads:
        load.start()

    def peer_at(d):
        far = nz // 2 - d // 2
        return lax.rem(seq + jnp.where(lax.rem(d, 2) == 1, far, nz - far), nz)

    def greet(d, _):
        pl.semaphore_signal(barrier, inc=1, device_id={"seq": peer_at(d)}, device_id_type=MESH)
        return 0

    lax.fori_loop(1, nz, greet, 0)
    for there in ({"blk": left}, {"blk": right}, {"cfg": 1 - cfg}):
        pl.semaphore_signal(barrier, inc=1, device_id=there, device_id_type=MESH)
    loads[0].wait()
    pl.semaphore_wait(barrier, nz + 2)

    def project(s, _):
        both = []
        for h in range(2):
            at = pl.ds(pl.multiple_of((2 * s + h) * HDIM, HDIM), HDIM)
            both.append(
                lax.dot_general(
                    v_ref[:, at], w_ref[:, at], (((1,), (1,)), ((), ())),
                    preferred_element_type=jnp.float32,
                )
            )
        vsend[s] = jnp.concatenate(both, axis=1).astype(jnp.bfloat16)
        return 0

    def columns(ref, first, count, s, h):
        return ref.at[pl.ds(first, count), pl.ds(pl.multiple_of((2 * s + h) * HDIM, HDIM), HDIM)]

    def source_place(n):
        return lax.rem(seq + jnp.where(lax.rem(n, 2) == 1, nz - (n + 1) // 2, n // 2), nz)

    def half_of(c, half):
        source = (lambda s: vsend.at[s]) if c == 1 else (lambda s: columns(k_ref, 0, tok, s, c // 2))
        return source, gx.at[c, blk, pl.ds(half * part, part), :], half

    def query_of(h):
        return lambda s: columns(q_ref, 0, tok, s, h), qx.at[h], None

    parcels = (
        half_of(0, 0), half_of(0, 1), half_of(1, 0), half_of(1, 1), query_of(0),
        half_of(2, 0), half_of(2, 1), query_of(1),
    )

    def spread(i):
        source, whole, half = parcels[i]

        def there(place):
            return whole.at[pl.ds(pl.multiple_of(place * tok, 16), tok), :]

        if half != 1:
            own = there(seq if half is None else 0)
            pltpu.make_async_copy(source(seq), own, zrecv.at[i]).start()

        def send(d, _):
            n = nz - d
            peer = source_place(n) if half is not None else peer_at(d)
            pltpu.make_async_remote_copy(
                src_ref=source(peer),
                dst_ref=there(seq if half is None else n - half * (nz // 2)),
                send_sem=zsend.at[i],
                recv_sem=zrecv.at[i],
                device_id={"seq": peer},
                device_id_type=MESH,
            ).start()
            return 0

        first, last = {None: (1, nz), 0: (nz // 2 + 1, nz), 1: (1, nz // 2 + 1)}[half]
        lax.fori_loop(first, last, send, 0)

    def spread_done(i):
        whole = parcels[i][1]
        pltpu.make_async_copy(whole, whole, zrecv.at[i]).wait()

    def ring(c, way, step, half):
        block = lax.rem(blk + (nx - step + 1 if way == 0 else step - 1), nx)
        piece = gx.at[c, block, pl.ds(half * part, part), :]
        return pltpu.make_async_remote_copy(
            src_ref=piece,
            dst_ref=piece,
            send_sem=xsend.at[c, way, step - 1, half],
            recv_sem=xrecv.at[c, way, step - 1, half],
            device_id={"blk": right if way == 0 else left},
            device_id_type=MESH,
        )

    def travels(way, step, half):
        return step < hops or (step == hops and way == half)

    def begin(c, half):
        for way in range(2):
            if travels(way, 1, half):
                ring(c, way, 1, half).start()

    def advance(c, step, half, way):
        if travels(way, step, half):
            ring(c, way, step, half).wait_recv()
            if travels(way, step + 1, half):
                ring(c, way, step + 1, half).start()

    qtile = rows // 2

    def attend(h, blocks):
        if h == 0:
            for block in blocks:
                turned = gx[1, block].T
                for g in range(2):
                    vt[block, g, pl.ds(0, patch), :] = turned[g * patch : (g + 1) * patch, :]
        items = [(block, t) for block in blocks for t in range(rows // qtile)]

        def scores_of(block, t):
            return lax.dot_general(
                gx[2 * h, block], qx[h, pl.ds(t * qtile, qtile), :], (((1,), (1,)), ((), ())),
                preferred_element_type=jnp.float32,
            )

        ahead = len(blocks)
        ready = [scores_of(*item) for item in items[:ahead]]
        for n, (block, t) in enumerate(items):
            if n + ahead < len(items):
                ready.append(scores_of(*items[n + ahead]))
            scores = ready.pop(0)
            at = pl.ds(t * qtile, qtile)
            old = top[h, :, at]
            new = jnp.maximum(old, jnp.max(scores, axis=0, keepdims=True))
            expo = jnp.exp2(scores * EXP_SCALE - new * EXP_SCALE).astype(jnp.bfloat16)
            factor = jnp.exp2((old - new) * EXP_SCALE)
            top[h, :, at] = new
            acc[h, :, at] = acc[h, :, at] * factor + jnp.dot(
                vt[block, h], expo, preferred_element_type=jnp.float32
            )

    spread(0)
    spread(1)
    loads[1].wait()
    loads[2].wait()
    lax.fori_loop(0, nz, project, 0)
    loads[3].wait()
    for i in range(2, len(parcels)):
        spread(i)
    top[...] = jnp.full(top.shape, -1e30, jnp.float32)
    acc[...] = jnp.zeros(acc.shape, jnp.float32)
    vt[:, :, pl.ds(patch, vt.shape[2] - patch), :] = jnp.ones(
        (nx, 2, vt.shape[2] - patch, rows), jnp.bfloat16
    )
    xcol[...] = jnp.zeros(xcol.shape, jnp.float32)
    loads[4].wait()
    wexp[...] = jnp.zeros(wexp.shape, jnp.bfloat16)
    for step_t in range(3):
        for step_y in range(3):
            taps = taps_ref[pl.ds((3 * step_t + step_y) * 3 * ZCH, 3 * ZCH), :]
            at = step_t * TAP_LANES + step_y * 4 * ZCH
            wexp[0, pl.ds(at + ZCH, 3 * ZCH), :] = taps
            wexp[1, pl.ds(at, 3 * ZCH), :] = taps

    for kind, c, *rest in ORDER:
        if kind == BEGIN:
            spread_done(((0, 1), (2, 3), (5, 6))[c][rest[0]])
            begin(c, rest[0])
        elif kind == QUERIES:
            spread_done((4, 7)[c])
        elif kind == PASS:
            step, half, way = rest
            for one in (0, 1) if way == BOTH else (way,):
                advance(c, step, half, one)
        else:
            attend(c, [lax.rem(blk + nx + rest[0], nx)])

    velocity = 0.0
    for h in range(2):
        velocity = velocity + acc[h, pl.ds(0, patch), :] / acc[h, pl.ds(patch, 1), :]
    velocity = velocity * jnp.where(cfg == 0, GUIDE, 1.0 - GUIDE)
    later = pltpu.roll(velocity, rows - few, 1)
    wide[...] = jnp.concatenate([velocity, later], axis=0).T

    def pack(s, _):
        vout[s] = wide[pl.ds(pl.multiple_of(s * tok, 16), few), :].astype(jnp.bfloat16)
        return 0

    lax.fori_loop(0, nz, pack, 0)
    slot = cfg * nz + seq

    def share(peer):
        return pltpu.make_async_remote_copy(
            src_ref=vout.at[peer],
            dst_ref=vin.at[slot],
            send_sem=vsent,
            recv_sem=vrecv,
            device_id={"seq": peer, "cfg": 1},
            device_id_type=MESH,
        )

    def send_share(d, _):
        share(peer_at(d)).start()
        return 0

    lax.fori_loop(1, nz, send_share, 0)

    @pl.when(cfg == 0)
    def _():
        share(seq).start()
        pltpu.make_async_copy(vout, vout, vsent).wait()

    def greater(target_cfg):
        return blk < frames if target_cfg == 0 else blk >= frames - 2

    @pl.when(cfg == 1)
    def _():
        pltpu.make_async_copy(vout.at[seq], vin.at[slot], vrecv).start()
        pltpu.make_async_copy(vin, vin, vrecv).wait()
        guided = jnp.sum(vin[...].astype(jnp.float32), axis=0)
        noisy = jnp.concatenate([noisy_ref[0:few, :], noisy_ref[few:tok, :]], axis=1)
        scale = jnp.concatenate([std_ref[...]] * (2 * patch // ZCH), axis=1)
        shift = jnp.concatenate([mean_ref[...]] * (2 * patch // ZCH), axis=1)
        pixels = (noisy - NOISE_LEVEL * guided) * scale + shift
        pixels = jnp.concatenate([pixels[:, :patch], pixels[:, patch:]], axis=0).astype(jnp.bfloat16)

        entry = lax.broadcasted_iota(jnp.int32, (patch, 2 * patch), 0)
        lane = lax.broadcasted_iota(jnp.int32, (patch, 2 * patch), 1)
        half = patch // 2
        spread_pixels = []
        for p in range(2):
            place = (
                (entry // half == lane // patch)
                & (entry % half == lane % half)
                & ((lane // half) % 2 == p)
            ).astype(jnp.bfloat16)
            spread_pixels.append(jnp.dot(pixels, place, preferred_element_type=jnp.float32))
        spread_pixels = jnp.concatenate(spread_pixels, axis=0).astype(jnp.bfloat16)
        slots = order_ref[...] - (blk * nz + seq) * tok
        slots = jnp.concatenate([slots, slots], axis=1)
        row = lax.broadcasted_iota(jnp.int32, (ROW_PAD * nx, 2 * tok), 0)
        token = lax.broadcasted_iota(jnp.int32, (ROW_PAD * nx, 2 * tok), 1)
        x = row % ROW_PAD
        column = COLS_DEV * (row // ROW_PAD) - 1 + (x + 1) // 2 + token // tok
        inside = (x < 2 * COLS_DEV) & (column >= 0) & (column < COLS_DEV * nx)
        for i in range(2):
            select = (inside & (slots == column + i * COLS_DEV * nx)).astype(jnp.bfloat16)
            picked = jnp.dot(select, spread_pixels, preferred_element_type=jnp.float32)
            psend[:, :, i * 2 * patch : (i + 1) * 2 * patch] = picked.reshape(
                nx, ROW_PAD, 2 * patch
            ).astype(jnp.bfloat16)

        above = lax.rem(seq + nz - 1, nz)
        below = lax.rem(seq + 1, nz)
        pieces = (
            (1, pl.ds(2 * patch, 2 * patch), halo.at[blk, 0], below),
            (1, pl.ds(0, 2 * patch), halo.at[blk, 1], above),
            (0, pl.ds(0, 4 * patch), tile.at[blk], seq),
        )
        for c in range(2):

            @pl.when(greater(c))
            def _():
                def send_pieces(d, _):
                    far = nx // 2 - d // 2
                    b = lax.rem(blk + jnp.where(lax.rem(d, 2) == 1, far, nx - far), nx)
                    for kind, at, there, s in pieces:
                        pltpu.make_async_remote_copy(
                            src_ref=psend.at[b, :, at],
                            dst_ref=there,
                            send_sem=psent.at[c, kind],
                            recv_sem=precv.at[kind],
                            device_id={"seq": s, "blk": b, "cfg": c},
                            device_id_type=MESH,
                        ).start()
                    return 0

                lax.fori_loop(1, nx, send_pieces, 0)
                for kind, at, there, s in pieces:
                    if c == 1 and kind == 0:
                        pltpu.make_async_copy(psend.at[blk, :, at], there, precv.at[0]).start()
                    else:
                        pltpu.make_async_remote_copy(
                            src_ref=psend.at[blk, :, at],
                            dst_ref=there,
                            send_sem=psent.at[c, kind],
                            recv_sem=precv.at[kind],
                            device_id={"seq": s, "cfg": c},
                            device_id_type=MESH,
                        ).start()

    for c in range(2):

        @pl.when(cfg == c)
        def _():
            arrived = pl.ds(0, frames) if c == 0 else pl.ds(frames - 2, frames + 2)
            pltpu.make_async_copy(tile.at[arrived], tile.at[arrived], precv.at[0]).wait()
            pltpu.make_async_copy(halo.at[arrived], halo.at[arrived], precv.at[1]).wait()

    def line(g, _):
        frame = cfg * frames - 2 + g
        known = frame >= 0
        frame = jnp.maximum(frame, 0)
        upper = halo[frame, 0].astype(jnp.float32)[:, patch:]
        lower = halo[frame, 1].astype(jnp.float32)[:, :patch]
        upper = jnp.where(known & (seq > 0), upper, 0.0)
        lower = jnp.where(known & (seq < nz - 1), lower, 0.0)
        middle = jnp.where(known, tile[frame].astype(jnp.float32), 0.0)
        grid[g] = jnp.concatenate([upper, middle, lower], axis=1)
        return 0

    lax.fori_loop(0, frames + 2, line, 0)
    for f in range(frames):
        for y in range(4):
            for step_t in range(3):
                xcol[pl.ds((4 * f + y) * ROW_PAD, ROW_PAD), pl.ds(step_t * TAP_LANES, 3 * patch)] = grid[
                    f + step_t, :, pl.ds(y * patch, 3 * patch)
                ]
    odd = lax.broadcasted_iota(jnp.int32, xcol.shape, 0) % 2 == 1
    features = 0.0
    for parity in range(2):
        kept = jnp.where(odd if parity else ~odd, xcol[...], 0.0).astype(jnp.bfloat16)
        features = features + jnp.dot(kept, wexp[parity], preferred_element_type=jnp.float32)
    wide_x = 2 * COLS_DEV
    to = lax.broadcasted_iota(jnp.int32, (frames * wide_x * 4, xcol.shape[0]), 0)
    at = lax.broadcasted_iota(jnp.int32, (frames * wide_x * 4, xcol.shape[0]), 1)
    source = ((to // (4 * wide_x)) * 4 + to % 4) * ROW_PAD + (to // 4) % wide_x
    order = (source == at).astype(jnp.bfloat16)
    upper = features.astype(jnp.bfloat16)
    lower = (features - upper.astype(jnp.float32)).astype(jnp.bfloat16)
    final[...] = jnp.dot(order, upper, preferred_element_type=jnp.float32) + jnp.dot(
        order, lower, preferred_element_type=jnp.float32
    )
    for f in range(frames):
        for x in range(wide_x):
            out_ref[f, x] = final[pl.ds((f * wide_x + x) * 4, 4), :]

    @pl.when(cfg == 1)
    def _():
        sent = vout.at[pl.ds(0, nz - 1)]
        pltpu.make_async_copy(sent, sent, vsent).wait()
        for c in range(2):

            @pl.when(greater(c))
            def _():
                tiles = psend.at[pl.ds(0, nx - c)]
                pltpu.make_async_copy(tiles, tiles, psent.at[c, 0]).wait()
                pltpu.make_async_copy(psend, psend, psent.at[c, 1]).wait()

    for i, (_, whole, half) in enumerate(parcels):
        sent = whole if half == 1 else whole.at[pl.ds(0, whole.shape[0] - tok), :]
        pltpu.make_async_copy(sent, sent, zsend.at[i]).wait()
    for c in range(3):
        for step in range(1, hops + 1):
            for half in range(2):
                for way in range(2):
                    if travels(way, step, half):
                        ring(c, way, step, half).wait_send()


def local(
    queries,
    key_states,
    value_states,
    noisy_latents,
    patch_order,
    head_weight,
    latent_std,
    latent_mean,
    conv_weight,
    conv_bias,
):
    nz = lax.axis_size("seq")
    nx = lax.axis_size("blk")
    tok = queries.shape[1]
    rows = nz * tok
    patch = head_weight.shape[1]
    wide = conv_weight.shape[4]
    frames = nx // 2
    pixels = 4 * frames * ROW_PAD
    vmem = pl.BlockSpec(memory_space=pltpu.VMEM)
    features = pl.pallas_call(
        functools.partial(exchange_kernel, nz, nx),
        out_shape=jax.ShapeDtypeStruct((frames, 2 * COLS_DEV, 4, wide), jnp.float32),
        in_specs=[pl.BlockSpec(memory_space=pl.ANY)] * 5 + [vmem] * 4,
        out_specs=vmem,
        scratch_shapes=[
            pltpu.VMEM(queries.shape[1:], jnp.bfloat16),
            pltpu.VMEM(queries.shape[1:], jnp.bfloat16),
            pltpu.VMEM(queries.shape[1:], jnp.bfloat16),
            pltpu.VMEM((patch, head_weight.shape[0]), jnp.bfloat16),
            pltpu.VMEM((27 * ZCH, wide), jnp.bfloat16),
            pltpu.VMEM((nz, tok, 2 * patch), jnp.bfloat16),
            pltpu.VMEM((3, nx, rows, HDIM), jnp.bfloat16),
            pltpu.VMEM((2, rows, HDIM), jnp.bfloat16),
            pltpu.VMEM((nx, 2, patch + ONES, rows), jnp.bfloat16),
            pltpu.VMEM((2, 1, rows), jnp.float32),
            pltpu.VMEM((2, patch + ONES, rows), jnp.float32),
            pltpu.VMEM((rows, 2 * patch), jnp.float32),
            pltpu.VMEM((nz, tok // 2, 2 * patch), jnp.bfloat16),
            pltpu.VMEM((2 * nz, tok // 2, 2 * patch), jnp.bfloat16),
            pltpu.VMEM((nx, ROW_PAD, 4 * patch), jnp.bfloat16),
            pltpu.VMEM((nx, ROW_PAD, 4 * patch), jnp.bfloat16),
            pltpu.VMEM((nx, 2, ROW_PAD, 2 * patch), jnp.bfloat16),
            pltpu.VMEM((frames + 2, ROW_PAD, 6 * patch), jnp.float32),
            pltpu.VMEM((pixels, 3 * TAP_LANES), jnp.float32),
            pltpu.VMEM((2, 3 * TAP_LANES, wide), jnp.bfloat16),
            pltpu.VMEM((8 * frames * COLS_DEV, wide), jnp.float32),
            pltpu.SemaphoreType.DMA((8,)),
            pltpu.SemaphoreType.DMA((8,)),
            pltpu.SemaphoreType.DMA((3, 2, nx // 2, 2)),
            pltpu.SemaphoreType.DMA((3, 2, nx // 2, 2)),
            pltpu.SemaphoreType.DMA,
            pltpu.SemaphoreType.DMA,
            pltpu.SemaphoreType.DMA((2, 2)),
            pltpu.SemaphoreType.DMA((2,)),
            pltpu.SemaphoreType.DMA((5,)),
        ],
        compiler_params=pltpu.CompilerParams(collective_id=0, has_side_effects=True),
    )(
        queries[0],
        key_states[0],
        value_states[0],
        head_weight.T,
        conv_weight.reshape(27 * ZCH, wide),
        noisy_latents,
        patch_order.reshape(1, tok),
        latent_std.reshape(1, ZCH),
        latent_mean.reshape(1, ZCH),
    )
    return (features + conv_bias).astype(jnp.bfloat16).transpose(0, 2, 1, 3)


def solution(mesh):
    in_specs = (
        P("cfg", ("prompt", "blk", "seq"), None),
        P("cfg", ("prompt", "blk", "seq"), None),
        P("cfg", ("prompt", "blk", "seq"), None),
        P(("prompt", "blk", "seq"), None),
        P(("prompt", "blk", "seq")),
        P(),
        P(),
        P(),
        P(),
        P(),
    )
    out_specs = P(("prompt", "cfg"), "seq", "blk", None)
    return jax.shard_map(local, mesh=mesh, in_specs=in_specs, out_specs=out_specs, check_vma=False)
```

```python
import functools
import math

import jax
import jax.numpy as jnp
from jax import lax
from jax.experimental import pallas as pl
from jax.experimental.pallas import tpu as pltpu
from jax.sharding import PartitionSpec as P

HDIM = 128
ZCH = 16
COLS_DEV = 3
ROW_PAD = 8
TAP_LANES = 256
ONES = 16
SPLIT = 2
GUIDE = 5.0
NOISE_LEVEL = 0.5
MESH = pl.DeviceIdType.MESH
BEGIN, QUERIES, PASS, ATTEND = range(4)
BOTH = 2
ORDER = (
    (BEGIN, 0, 0), (PASS, 0, 1, 0, BOTH), (BEGIN, 0, 1), (PASS, 0, 2, 0, BOTH), (BEGIN, 1, 0),
    (PASS, 0, 1, 1, BOTH), (PASS, 0, 3, 0, BOTH), (PASS, 1, 1, 0, BOTH), (BEGIN, 1, 1),
    (PASS, 0, 2, 1, BOTH), (BEGIN, 2, 0), (PASS, 0, 4, 0, 0), (PASS, 1, 2, 0, BOTH),
    (PASS, 1, 1, 1, BOTH), (PASS, 0, 3, 1, 1), (BEGIN, 2, 1), (PASS, 0, 3, 1, 0),
    (PASS, 2, 1, 0, BOTH), (PASS, 1, 3, 0, BOTH), (PASS, 1, 2, 1, BOTH), (PASS, 0, 4, 1, 1),
    (QUERIES, 0), (ATTEND, 0, 0), (PASS, 2, 1, 1, BOTH), (ATTEND, 0, -1), (ATTEND, 0, 1),
    (PASS, 2, 2, 0, BOTH), (ATTEND, 0, -2), (ATTEND, 0, 2), (PASS, 1, 4, 0, 0), (PASS, 1, 3, 1, 1),
    (ATTEND, 0, 3), (PASS, 1, 3, 1, 0), (PASS, 2, 2, 1, 1), (ATTEND, 0, -3), (QUERIES, 1),
    (ATTEND, 1, 0), (PASS, 2, 2, 1, 0), (PASS, 2, 3, 0, 1), (ATTEND, 1, -1), (ATTEND, 1, 1),
    (PASS, 2, 3, 0, 0), (PASS, 1, 4, 1, 1), (ATTEND, 0, 4), (ATTEND, 1, -2), (PASS, 2, 3, 1, BOTH),
    (ATTEND, 1, 2), (ATTEND, 1, -3), (PASS, 2, 4, 0, 0), (ATTEND, 1, 3), (PASS, 2, 4, 1, 1),
    (ATTEND, 1, 4),
)
EXP_SCALE = math.log2(math.e) / math.sqrt(HDIM)


def exchange_kernel(
    nz, nx, q_hbm, k_hbm, v_hbm, w_hbm, taps_hbm, noisy_ref, order_ref, std_ref, mean_ref, out_ref,
    q_ref, k_ref, v_ref, w_ref, taps_ref,
    vsend, gx, qx, vt, top, acc, wide, vout, vin, psend, tile, halo, grid, xcol, wexp, final,
    zsend, zrecv, xsend, xrecv, vsent, vrecv, psent, precv, loaded,
):
    seq = lax.axis_index("seq")
    blk = lax.axis_index("blk")
    cfg = lax.axis_index("cfg")
    tok = q_ref.shape[0]
    rows = gx.shape[2]
    part = rows // 2
    patch = w_ref.shape[0]
    frames = nx // 2
    few = tok // 2
    hops = nx // 2
    right = lax.rem(blk + 1, nx)
    left = lax.rem(blk + nx - 1, nx)

    barrier = pltpu.get_barrier_semaphore()

    loads = [
        pltpu.make_async_copy(there, here, loaded.at[n])
        for n, (there, here) in enumerate(
            ((k_hbm, k_ref), (v_hbm, v_ref), (w_hbm, w_ref), (q_hbm, q_ref), (taps_hbm, taps_ref))
        )
    ]
    for load in loads:
        load.start()

    def peer_at(d):
        far = nz // 2 - d // 2
        return lax.rem(seq + jnp.where(lax.rem(d, 2) == 1, far, nz - far), nz)

    def greet(d, _):
        pl.semaphore_signal(barrier, inc=1, device_id={"seq": peer_at(d)}, device_id_type=MESH)
        return 0

    lax.fori_loop(1, nz, greet, 0)
    for there in ({"blk": left}, {"blk": right}, {"cfg": 1 - cfg}):
        pl.semaphore_signal(barrier, inc=1, device_id=there, device_id_type=MESH)
    loads[0].wait()
    pl.semaphore_wait(barrier, nz + 2)

    def project(s, _):
        both = []
        for h in range(2):
            at = pl.ds(pl.multiple_of((2 * s + h) * HDIM, HDIM), HDIM)
            both.append(
                lax.dot_general(
                    v_ref[:, at], w_ref[:, at], (((1,), (1,)), ((), ())),
                    preferred_element_type=jnp.float32,
                )
            )
        vsend[s] = jnp.concatenate(both, axis=1).astype(jnp.bfloat16)
        return 0

    def columns(ref, first, count, s, h):
        return ref.at[pl.ds(first, count), pl.ds(pl.multiple_of((2 * s + h) * HDIM, HDIM), HDIM)]

    def source_place(n):
        return lax.rem(seq + jnp.where(lax.rem(n, 2) == 1, nz - (n + 1) // 2, n // 2), nz)

    def half_of(c, half):
        source = (lambda s: vsend.at[s]) if c == 1 else (lambda s: columns(k_ref, 0, tok, s, c // 2))
        return source, gx.at[c, blk, pl.ds(half * part, part), :], half

    def query_of(h):
        return lambda s: columns(q_ref, 0, tok, s, h), qx.at[h], None

    parcels = (
        half_of(0, 0), half_of(0, 1), half_of(1, 0), half_of(1, 1),
        half_of(2, 0), half_of(2, 1), query_of(0), query_of(1),
    )

    def spread(i):
        source, whole, half = parcels[i]

        def there(place):
            return whole.at[pl.ds(pl.multiple_of(place * tok, 16), tok), :]

        if half != 1:
            own = there(seq if half is None else 0)
            pltpu.make_async_copy(source(seq), own, zrecv.at[i]).start()

        def send(d, _):
            n = nz - d
            peer = source_place(n) if half is not None else peer_at(d)
            pltpu.make_async_remote_copy(
                src_ref=source(peer),
                dst_ref=there(seq if half is None else n - half * (nz // 2)),
                send_sem=zsend.at[i],
                recv_sem=zrecv.at[i],
                device_id={"seq": peer},
                device_id_type=MESH,
            ).start()
            return 0

        first, last = {None: (1, nz), 0: (nz // 2 + 1, nz), 1: (1, nz // 2 + 1)}[half]
        lax.fori_loop(first, last, send, 0)

    def spread_done(i):
        whole = parcels[i][1]
        pltpu.make_async_copy(whole, whole, zrecv.at[i]).wait()

    def ring(c, way, step, half, piece):
        block = lax.rem(blk + (nx - step + 1 if way == 0 else step - 1), nx)
        count = part // SPLIT
        slot = half * SPLIT + piece
        moved = gx.at[c, block, pl.ds(slot * count, count), :]
        return pltpu.make_async_remote_copy(
            src_ref=moved,
            dst_ref=moved,
            send_sem=xsend.at[c, way, step - 1, slot],
            recv_sem=xrecv.at[c, way, step - 1, slot],
            device_id={"blk": right if way == 0 else left},
            device_id_type=MESH,
        )

    def travels(way, step, half):
        return step < hops or (step == hops and way == half)

    def begin(c, half):
        for piece in range(SPLIT):
            for way in range(2):
                if travels(way, 1, half):
                    ring(c, way, 1, half, piece).start()

    def advance(c, step, half, ways):
        for piece in range(SPLIT):
            for way in ways:
                if travels(way, step, half):
                    ring(c, way, step, half, piece).wait_recv()
                    if travels(way, step + 1, half):
                        ring(c, way, step + 1, half, piece).start()

    qtile = rows // 2

    def attend(h, blocks):
        if h == 0:
            for block in blocks:
                turned = gx[1, block].T
                for g in range(2):
                    vt[block, g, pl.ds(0, patch), :] = turned[g * patch : (g + 1) * patch, :]
        items = [(block, t) for block in blocks for t in range(rows // qtile)]

        def scores_of(block, t):
            return lax.dot_general(
                gx[2 * h, block], qx[h, pl.ds(t * qtile, qtile), :], (((1,), (1,)), ((), ())),
                preferred_element_type=jnp.float32,
            )

        ahead = len(blocks)
        ready = [scores_of(*item) for item in items[:ahead]]
        for n, (block, t) in enumerate(items):
            if n + ahead < len(items):
                ready.append(scores_of(*items[n + ahead]))
            scores = ready.pop(0)
            at = pl.ds(t * qtile, qtile)
            old = top[h, :, at]
            new = jnp.maximum(old, jnp.max(scores, axis=0, keepdims=True))
            expo = jnp.exp2(scores * EXP_SCALE - new * EXP_SCALE).astype(jnp.bfloat16)
            factor = jnp.exp2((old - new) * EXP_SCALE)
            top[h, :, at] = new
            acc[h, :, at] = acc[h, :, at] * factor + jnp.dot(
                vt[block, h], expo, preferred_element_type=jnp.float32
            )

    spread(0)
    spread(1)
    loads[1].wait()
    loads[2].wait()
    lax.fori_loop(0, nz, project, 0)
    loads[3].wait()
    for i in range(2, len(parcels)):
        spread(i)
    top[...] = jnp.full(top.shape, -1e30, jnp.float32)
    acc[...] = jnp.zeros(acc.shape, jnp.float32)
    vt[:, :, pl.ds(patch, vt.shape[2] - patch), :] = jnp.ones(
        (nx, 2, vt.shape[2] - patch, rows), jnp.bfloat16
    )
    xcol[...] = jnp.zeros(xcol.shape, jnp.float32)
    loads[4].wait()
    wexp[...] = jnp.zeros(wexp.shape, jnp.bfloat16)
    for step_t in range(3):
        for step_y in range(3):
            taps = taps_ref[pl.ds((3 * step_t + step_y) * 3 * ZCH, 3 * ZCH), :]
            at = step_t * TAP_LANES + step_y * 4 * ZCH
            wexp[0, pl.ds(at + ZCH, 3 * ZCH), :] = taps
            wexp[1, pl.ds(at, 3 * ZCH), :] = taps

    for kind, c, *rest in ORDER:
        if kind == BEGIN:
            spread_done(2 * c + rest[0])
            begin(c, rest[0])
        elif kind == QUERIES:
            spread_done(6 + c)
        elif kind == PASS:
            step, half, way = rest
            advance(c, step, half, (0, 1) if way == BOTH else (way,))
        else:
            attend(c, [lax.rem(blk + nx + rest[0], nx)])

    velocity = 0.0
    for h in range(2):
        velocity = velocity + acc[h, pl.ds(0, patch), :] / acc[h, pl.ds(patch, 1), :]
    velocity = velocity * jnp.where(cfg == 0, GUIDE, 1.0 - GUIDE)
    later = pltpu.roll(velocity, rows - few, 1)
    wide[...] = jnp.concatenate([velocity, later], axis=0).T

    def pack(s, _):
        vout[s] = wide[pl.ds(pl.multiple_of(s * tok, 16), few), :].astype(jnp.bfloat16)
        return 0

    lax.fori_loop(0, nz, pack, 0)
    slot = cfg * nz + seq

    def share(peer):
        return pltpu.make_async_remote_copy(
            src_ref=vout.at[peer],
            dst_ref=vin.at[slot],
            send_sem=vsent,
            recv_sem=vrecv,
            device_id={"seq": peer, "cfg": 1},
            device_id_type=MESH,
        )

    def send_share(d, _):
        share(peer_at(d)).start()
        return 0

    lax.fori_loop(1, nz, send_share, 0)

    @pl.when(cfg == 0)
    def _():
        share(seq).start()
        pltpu.make_async_copy(vout, vout, vsent).wait()

    def greater(target_cfg):
        return blk < frames if target_cfg == 0 else blk >= frames - 2

    @pl.when(cfg == 1)
    def _():
        pltpu.make_async_copy(vout.at[seq], vin.at[slot], vrecv).start()
        pltpu.make_async_copy(vin, vin, vrecv).wait()
        guided = jnp.sum(vin[...].astype(jnp.float32), axis=0)
        noisy = jnp.concatenate([noisy_ref[0:few, :], noisy_ref[few:tok, :]], axis=1)
        scale = jnp.concatenate([std_ref[...]] * (2 * patch // ZCH), axis=1)
        shift = jnp.concatenate([mean_ref[...]] * (2 * patch // ZCH), axis=1)
        pixels = (noisy - NOISE_LEVEL * guided) * scale + shift
        pixels = jnp.concatenate([pixels[:, :patch], pixels[:, patch:]], axis=0).astype(jnp.bfloat16)

        entry = lax.broadcasted_iota(jnp.int32, (patch, 2 * patch), 0)
        lane = lax.broadcasted_iota(jnp.int32, (patch, 2 * patch), 1)
        half = patch // 2
        spread_pixels = []
        for p in range(2):
            place = (
                (entry // half == lane // patch)
                & (entry % half == lane % half)
                & ((lane // half) % 2 == p)
            ).astype(jnp.bfloat16)
            spread_pixels.append(jnp.dot(pixels, place, preferred_element_type=jnp.float32))
        spread_pixels = jnp.concatenate(spread_pixels, axis=0).astype(jnp.bfloat16)
        slots = order_ref[...] - (blk * nz + seq) * tok
        slots = jnp.concatenate([slots, slots], axis=1)
        row = lax.broadcasted_iota(jnp.int32, (ROW_PAD * nx, 2 * tok), 0)
        token = lax.broadcasted_iota(jnp.int32, (ROW_PAD * nx, 2 * tok), 1)
        x = row % ROW_PAD
        column = COLS_DEV * (row // ROW_PAD) - 1 + (x + 1) // 2 + token // tok
        inside = (x < 2 * COLS_DEV) & (column >= 0) & (column < COLS_DEV * nx)
        for i in range(2):
            select = (inside & (slots == column + i * COLS_DEV * nx)).astype(jnp.bfloat16)
            picked = jnp.dot(select, spread_pixels, preferred_element_type=jnp.float32)
            psend[:, :, i * 2 * patch : (i + 1) * 2 * patch] = picked.reshape(
                nx, ROW_PAD, 2 * patch
            ).astype(jnp.bfloat16)

        above = lax.rem(seq + nz - 1, nz)
        below = lax.rem(seq + 1, nz)
        pieces = (
            (1, pl.ds(2 * patch, 2 * patch), halo.at[blk, 0], below),
            (1, pl.ds(0, 2 * patch), halo.at[blk, 1], above),
            (0, pl.ds(0, 4 * patch), tile.at[blk], seq),
        )
        for c in range(2):

            @pl.when(greater(c))
            def _():
                def send_pieces(d, _):
                    far = nx // 2 - d // 2
                    b = lax.rem(blk + jnp.where(lax.rem(d, 2) == 1, far, nx - far), nx)
                    for kind, at, there, s in pieces:
                        pltpu.make_async_remote_copy(
                            src_ref=psend.at[b, :, at],
                            dst_ref=there,
                            send_sem=psent.at[c, kind],
                            recv_sem=precv.at[kind],
                            device_id={"seq": s, "blk": b, "cfg": c},
                            device_id_type=MESH,
                        ).start()
                    return 0

                lax.fori_loop(1, nx, send_pieces, 0)
                for kind, at, there, s in pieces:
                    if c == 1 and kind == 0:
                        pltpu.make_async_copy(psend.at[blk, :, at], there, precv.at[0]).start()
                    else:
                        pltpu.make_async_remote_copy(
                            src_ref=psend.at[blk, :, at],
                            dst_ref=there,
                            send_sem=psent.at[c, kind],
                            recv_sem=precv.at[kind],
                            device_id={"seq": s, "cfg": c},
                            device_id_type=MESH,
                        ).start()

    for c in range(2):

        @pl.when(cfg == c)
        def _():
            arrived = pl.ds(0, frames) if c == 0 else pl.ds(frames - 2, frames + 2)
            pltpu.make_async_copy(tile.at[arrived], tile.at[arrived], precv.at[0]).wait()
            pltpu.make_async_copy(halo.at[arrived], halo.at[arrived], precv.at[1]).wait()

    def line(g, _):
        frame = cfg * frames - 2 + g
        known = frame >= 0
        frame = jnp.maximum(frame, 0)
        upper = halo[frame, 0].astype(jnp.float32)[:, patch:]
        lower = halo[frame, 1].astype(jnp.float32)[:, :patch]
        upper = jnp.where(known & (seq > 0), upper, 0.0)
        lower = jnp.where(known & (seq < nz - 1), lower, 0.0)
        middle = jnp.where(known, tile[frame].astype(jnp.float32), 0.0)
        grid[g] = jnp.concatenate([upper, middle, lower], axis=1)
        return 0

    lax.fori_loop(0, frames + 2, line, 0)
    for f in range(frames):
        for y in range(4):
            for step_t in range(3):
                xcol[pl.ds((4 * f + y) * ROW_PAD, ROW_PAD), pl.ds(step_t * TAP_LANES, 3 * patch)] = grid[
                    f + step_t, :, pl.ds(y * patch, 3 * patch)
                ]
    odd = lax.broadcasted_iota(jnp.int32, xcol.shape, 0) % 2 == 1
    features = 0.0
    for parity in range(2):
        kept = jnp.where(odd if parity else ~odd, xcol[...], 0.0).astype(jnp.bfloat16)
        features = features + jnp.dot(kept, wexp[parity], preferred_element_type=jnp.float32)
    wide_x = 2 * COLS_DEV
    to = lax.broadcasted_iota(jnp.int32, (frames * wide_x * 4, xcol.shape[0]), 0)
    at = lax.broadcasted_iota(jnp.int32, (frames * wide_x * 4, xcol.shape[0]), 1)
    source = ((to // (4 * wide_x)) * 4 + to % 4) * ROW_PAD + (to // 4) % wide_x
    order = (source == at).astype(jnp.bfloat16)
    upper = features.astype(jnp.bfloat16)
    lower = (features - upper.astype(jnp.float32)).astype(jnp.bfloat16)
    final[...] = jnp.dot(order, upper, preferred_element_type=jnp.float32) + jnp.dot(
        order, lower, preferred_element_type=jnp.float32
    )
    for f in range(frames):
        for x in range(wide_x):
            out_ref[f, x] = final[pl.ds((f * wide_x + x) * 4, 4), :]

    @pl.when(cfg == 1)
    def _():
        sent = vout.at[pl.ds(0, nz - 1)]
        pltpu.make_async_copy(sent, sent, vsent).wait()
        for c in range(2):

            @pl.when(greater(c))
            def _():
                tiles = psend.at[pl.ds(0, nx - c)]
                pltpu.make_async_copy(tiles, tiles, psent.at[c, 0]).wait()
                pltpu.make_async_copy(psend, psend, psent.at[c, 1]).wait()

    for i, (_, whole, half) in enumerate(parcels):
        sent = whole if half == 1 else whole.at[pl.ds(0, whole.shape[0] - tok), :]
        pltpu.make_async_copy(sent, sent, zsend.at[i]).wait()
    for c in range(3):
        for step in range(1, hops + 1):
            for half in range(2):
                for way in range(2):
                    for piece in range(SPLIT if travels(way, step, half) else 0):
                        ring(c, way, step, half, piece).wait_send()


def local(
    queries,
    key_states,
    value_states,
    noisy_latents,
    patch_order,
    head_weight,
    latent_std,
    latent_mean,
    conv_weight,
    conv_bias,
):
    nz = lax.axis_size("seq")
    nx = lax.axis_size("blk")
    tok = queries.shape[1]
    rows = nz * tok
    patch = head_weight.shape[1]
    wide = conv_weight.shape[4]
    frames = nx // 2
    pixels = 4 * frames * ROW_PAD
    vmem = pl.BlockSpec(memory_space=pltpu.VMEM)
    features = pl.pallas_call(
        functools.partial(exchange_kernel, nz, nx),
        out_shape=jax.ShapeDtypeStruct((frames, 2 * COLS_DEV, 4, wide), jnp.float32),
        in_specs=[pl.BlockSpec(memory_space=pl.ANY)] * 5 + [vmem] * 4,
        out_specs=vmem,
        scratch_shapes=[
            pltpu.VMEM(queries.shape[1:], jnp.bfloat16),
            pltpu.VMEM(queries.shape[1:], jnp.bfloat16),
            pltpu.VMEM(queries.shape[1:], jnp.bfloat16),
            pltpu.VMEM((patch, head_weight.shape[0]), jnp.bfloat16),
            pltpu.VMEM((27 * ZCH, wide), jnp.bfloat16),
            pltpu.VMEM((nz, tok, 2 * patch), jnp.bfloat16),
            pltpu.VMEM((3, nx, rows, HDIM), jnp.bfloat16),
            pltpu.VMEM((2, rows, HDIM), jnp.bfloat16),
            pltpu.VMEM((nx, 2, patch + ONES, rows), jnp.bfloat16),
            pltpu.VMEM((2, 1, rows), jnp.float32),
            pltpu.VMEM((2, patch + ONES, rows), jnp.float32),
            pltpu.VMEM((rows, 2 * patch), jnp.float32),
            pltpu.VMEM((nz, tok // 2, 2 * patch), jnp.bfloat16),
            pltpu.VMEM((2 * nz, tok // 2, 2 * patch), jnp.bfloat16),
            pltpu.VMEM((nx, ROW_PAD, 4 * patch), jnp.bfloat16),
            pltpu.VMEM((nx, ROW_PAD, 4 * patch), jnp.bfloat16),
            pltpu.VMEM((nx, 2, ROW_PAD, 2 * patch), jnp.bfloat16),
            pltpu.VMEM((frames + 2, ROW_PAD, 6 * patch), jnp.float32),
            pltpu.VMEM((pixels, 3 * TAP_LANES), jnp.float32),
            pltpu.VMEM((2, 3 * TAP_LANES, wide), jnp.bfloat16),
            pltpu.VMEM((8 * frames * COLS_DEV, wide), jnp.float32),
            pltpu.SemaphoreType.DMA((8,)),
            pltpu.SemaphoreType.DMA((8,)),
            pltpu.SemaphoreType.DMA((3, 2, nx // 2, 2 * SPLIT)),
            pltpu.SemaphoreType.DMA((3, 2, nx // 2, 2 * SPLIT)),
            pltpu.SemaphoreType.DMA,
            pltpu.SemaphoreType.DMA,
            pltpu.SemaphoreType.DMA((2, 2)),
            pltpu.SemaphoreType.DMA((2,)),
            pltpu.SemaphoreType.DMA((5,)),
        ],
        compiler_params=pltpu.CompilerParams(collective_id=0, has_side_effects=True),
    )(
        queries[0],
        key_states[0],
        value_states[0],
        head_weight.T,
        conv_weight.reshape(27 * ZCH, wide),
        noisy_latents,
        patch_order.reshape(1, tok),
        latent_std.reshape(1, ZCH),
        latent_mean.reshape(1, ZCH),
    )
    return (features + conv_bias).astype(jnp.bfloat16).transpose(0, 2, 1, 3)


def solution(mesh):
    in_specs = (
        P("cfg", ("prompt", "blk", "seq"), None),
        P("cfg", ("prompt", "blk", "seq"), None),
        P("cfg", ("prompt", "blk", "seq"), None),
        P(("prompt", "blk", "seq"), None),
        P(("prompt", "blk", "seq")),
        P(),
        P(),
        P(),
        P(),
        P(),
    )
    out_specs = P(("prompt", "cfg"), "seq", "blk", None)
    return jax.shard_map(local, mesh=mesh, in_specs=in_specs, out_specs=out_specs, check_vma=False)
```

```python
import functools
import math

import jax
import jax.numpy as jnp
from jax import lax
from jax.experimental import pallas as pl
from jax.experimental.pallas import tpu as pltpu
from jax.sharding import PartitionSpec as P

HDIM = 128
ZCH = 16
COLS_DEV = 3
ROW_PAD = 8
TAP_LANES = 256
ONES = 16
SPLIT = 2
VMEM_LIMIT = 55000 * 1024
GUIDE = 5.0
NOISE_LEVEL = 0.5
MESH = pl.DeviceIdType.MESH
BEGIN, QUERIES, PASS, ATTEND = range(4)
BOTH = 2
ORDER = (
    (BEGIN, 0, 0), (PASS, 0, 1, 0, BOTH), (BEGIN, 0, 1), (PASS, 0, 2, 0, BOTH), (BEGIN, 1, 0),
    (PASS, 0, 1, 1, BOTH), (PASS, 0, 3, 0, BOTH), (PASS, 1, 1, 0, BOTH), (BEGIN, 1, 1),
    (PASS, 0, 2, 1, BOTH), (BEGIN, 2, 0), (PASS, 0, 4, 0, 0), (PASS, 1, 2, 0, BOTH),
    (PASS, 1, 1, 1, BOTH), (PASS, 0, 3, 1, 1), (BEGIN, 2, 1), (PASS, 0, 3, 1, 0),
    (PASS, 2, 1, 0, BOTH), (PASS, 1, 3, 0, BOTH), (PASS, 1, 2, 1, BOTH), (PASS, 0, 4, 1, 1),
    (QUERIES, 0), (ATTEND, 0, 0), (PASS, 2, 1, 1, BOTH), (ATTEND, 0, -1), (ATTEND, 0, 1),
    (PASS, 2, 2, 0, BOTH), (ATTEND, 0, -2), (ATTEND, 0, 2), (PASS, 1, 4, 0, 0), (PASS, 1, 3, 1, 1),
    (ATTEND, 0, 3), (PASS, 1, 3, 1, 0), (PASS, 2, 2, 1, 1), (ATTEND, 0, -3), (QUERIES, 1),
    (ATTEND, 1, 0), (PASS, 2, 2, 1, 0), (PASS, 2, 3, 0, 1), (ATTEND, 1, -1), (ATTEND, 1, 1),
    (PASS, 2, 3, 0, 0), (PASS, 1, 4, 1, 1), (ATTEND, 0, 4), (ATTEND, 1, -2), (PASS, 2, 3, 1, BOTH),
    (ATTEND, 1, 2), (ATTEND, 1, -3), (PASS, 2, 4, 0, 0), (ATTEND, 1, 3), (PASS, 2, 4, 1, 1),
    (ATTEND, 1, 4),
)
EXP_SCALE = math.log2(math.e) / math.sqrt(HDIM)


def exchange_kernel(
    nz, nx, q_hbm, k_hbm, v_hbm, w_hbm, taps_hbm, noisy_ref, order_ref, std_ref, mean_ref, out_ref,
    q_ref, k_ref, v_ref, w_ref, taps_ref,
    vsend, gx, qx, vt, top, acc, wide, vout, vin, psend, tile, halo, grid, xcol, wexp, final,
    zsend, zrecv, xsend, xrecv, vsent, vrecv, psent, precv, loaded,
):
    seq = lax.axis_index("seq")
    blk = lax.axis_index("blk")
    cfg = lax.axis_index("cfg")
    tok = q_ref.shape[0]
    rows = gx.shape[2]
    part = rows // 2
    patch = w_ref.shape[0]
    frames = nx // 2
    few = tok // 2
    hops = nx // 2
    right = lax.rem(blk + 1, nx)
    left = lax.rem(blk + nx - 1, nx)

    barrier = pltpu.get_barrier_semaphore()

    loads = [
        pltpu.make_async_copy(there, here, loaded.at[n])
        for n, (there, here) in enumerate(
            ((k_hbm, k_ref), (v_hbm, v_ref), (w_hbm, w_ref), (q_hbm, q_ref), (taps_hbm, taps_ref))
        )
    ]
    for load in loads:
        load.start()

    def peer_at(d):
        far = nz // 2 - d // 2
        return lax.rem(seq + jnp.where(lax.rem(d, 2) == 1, far, nz - far), nz)

    def greet(d, _):
        pl.semaphore_signal(barrier, inc=1, device_id={"seq": peer_at(d)}, device_id_type=MESH)
        return 0

    lax.fori_loop(1, nz, greet, 0)
    for there in ({"blk": left}, {"blk": right}, {"cfg": 1 - cfg}):
        pl.semaphore_signal(barrier, inc=1, device_id=there, device_id_type=MESH)
    loads[0].wait()
    pl.semaphore_wait(barrier, nz + 2)

    def project(s, _):
        both = []
        for h in range(2):
            at = pl.ds(pl.multiple_of((2 * s + h) * HDIM, HDIM), HDIM)
            both.append(
                lax.dot_general(
                    v_ref[:, at], w_ref[:, at], (((1,), (1,)), ((), ())),
                    preferred_element_type=jnp.float32,
                )
            )
        vsend[s] = jnp.concatenate(both, axis=1).astype(jnp.bfloat16)
        return 0

    def columns(ref, first, count, s, h):
        return ref.at[pl.ds(first, count), pl.ds(pl.multiple_of((2 * s + h) * HDIM, HDIM), HDIM)]

    def source_place(n):
        return lax.rem(seq + jnp.where(lax.rem(n, 2) == 1, nz - (n + 1) // 2, n // 2), nz)

    def half_of(c, half):
        source = (lambda s: vsend.at[s]) if c == 1 else (lambda s: columns(k_ref, 0, tok, s, c // 2))
        return source, gx.at[c, blk, pl.ds(half * part, part), :], half

    def query_of(h):
        return lambda s: columns(q_ref, 0, tok, s, h), qx.at[h], None

    parcels = (
        half_of(0, 0), half_of(0, 1), half_of(1, 0), half_of(1, 1),
        half_of(2, 0), half_of(2, 1), query_of(0), query_of(1),
    )

    def spread(i):
        source, whole, half = parcels[i]

        def there(place):
            return whole.at[pl.ds(pl.multiple_of(place * tok, 16), tok), :]

        if half != 1:
            own = there(seq if half is None else 0)
            pltpu.make_async_copy(source(seq), own, zrecv.at[i]).start()

        def send(d, _):
            n = nz - d
            peer = source_place(n) if half is not None else peer_at(d)
            pltpu.make_async_remote_copy(
                src_ref=source(peer),
                dst_ref=there(seq if half is None else n - half * (nz // 2)),
                send_sem=zsend.at[i],
                recv_sem=zrecv.at[i],
                device_id={"seq": peer},
                device_id_type=MESH,
            ).start()
            return 0

        first, last = {None: (1, nz), 0: (nz // 2 + 1, nz), 1: (1, nz // 2 + 1)}[half]
        lax.fori_loop(first, last, send, 0)

    def spread_done(i):
        whole = parcels[i][1]
        pltpu.make_async_copy(whole, whole, zrecv.at[i]).wait()

    def ring(c, way, step, half, piece):
        block = lax.rem(blk + (nx - step + 1 if way == 0 else step - 1), nx)
        count = part // SPLIT
        slot = half * SPLIT + piece
        moved = gx.at[c, block, pl.ds(slot * count, count), :]
        return pltpu.make_async_remote_copy(
            src_ref=moved,
            dst_ref=moved,
            send_sem=xsend.at[c, way, step - 1, slot],
            recv_sem=xrecv.at[c, way, step - 1, slot],
            device_id={"blk": right if way == 0 else left},
            device_id_type=MESH,
        )

    def travels(way, step, half):
        return step < hops or (step == hops and way == half)

    def begin(c, half):
        for piece in range(SPLIT):
            for way in range(2):
                if travels(way, 1, half):
                    ring(c, way, 1, half, piece).start()

    def advance(c, step, half, ways):
        for piece in range(SPLIT):
            for way in ways:
                if travels(way, step, half):
                    ring(c, way, step, half, piece).wait_recv()
                    if travels(way, step + 1, half):
                        ring(c, way, step + 1, half, piece).start()

    qtile = rows // 2

    def attend(h, blocks):
        if h == 0:
            for block in blocks:
                turned = gx[1, block].T
                for g in range(2):
                    vt[block, g, pl.ds(0, patch), :] = turned[g * patch : (g + 1) * patch, :]
        items = [(block, t) for block in blocks for t in range(rows // qtile)]

        def scores_of(block, t):
            return lax.dot_general(
                gx[2 * h, block], qx[h, pl.ds(t * qtile, qtile), :], (((1,), (1,)), ((), ())),
                preferred_element_type=jnp.float32,
            )

        ahead = len(blocks)
        ready = [scores_of(*item) for item in items[:ahead]]
        for n, (block, t) in enumerate(items):
            if n + ahead < len(items):
                ready.append(scores_of(*items[n + ahead]))
            scores = ready.pop(0)
            at = pl.ds(t * qtile, qtile)
            old = top[h, :, at]
            new = jnp.maximum(old, jnp.max(scores, axis=0, keepdims=True))
            expo = jnp.exp2(scores * EXP_SCALE - new * EXP_SCALE).astype(jnp.bfloat16)
            factor = jnp.exp2((old - new) * EXP_SCALE)
            top[h, :, at] = new
            acc[h, :, at] = acc[h, :, at] * factor + jnp.dot(
                vt[block, h], expo, preferred_element_type=jnp.float32
            )

    spread(0)
    spread(1)
    loads[1].wait()
    loads[2].wait()
    lax.fori_loop(0, nz, project, 0)
    loads[3].wait()
    for i in range(2, len(parcels)):
        spread(i)
    top[...] = jnp.full(top.shape, -1e30, jnp.float32)
    acc[...] = jnp.zeros(acc.shape, jnp.float32)
    vt[:, :, pl.ds(patch, vt.shape[2] - patch), :] = jnp.ones(
        (nx, 2, vt.shape[2] - patch, rows), jnp.bfloat16
    )
    xcol[...] = jnp.zeros(xcol.shape, jnp.float32)
    loads[4].wait()
    wexp[...] = jnp.zeros(wexp.shape, jnp.bfloat16)
    for step_t in range(3):
        for step_y in range(3):
            taps = taps_ref[pl.ds((3 * step_t + step_y) * 3 * ZCH, 3 * ZCH), :]
            at = step_t * TAP_LANES + step_y * 4 * ZCH
            wexp[0, pl.ds(at + ZCH, 3 * ZCH), :] = taps
            wexp[1, pl.ds(at, 3 * ZCH), :] = taps

    for kind, c, *rest in ORDER:
        if kind == BEGIN:
            spread_done(2 * c + rest[0])
            begin(c, rest[0])
        elif kind == QUERIES:
            spread_done(6 + c)
        elif kind == PASS:
            step, half, way = rest
            advance(c, step, half, (0, 1) if way == BOTH else (way,))
        else:
            attend(c, [lax.rem(blk + nx + rest[0], nx)])

    velocity = 0.0
    for h in range(2):
        velocity = velocity + acc[h, pl.ds(0, patch), :] / acc[h, pl.ds(patch, 1), :]
    velocity = velocity * jnp.where(cfg == 0, GUIDE, 1.0 - GUIDE)
    later = pltpu.roll(velocity, rows - few, 1)
    wide[...] = jnp.concatenate([velocity, later], axis=0).T

    def pack(s, _):
        vout[s] = wide[pl.ds(pl.multiple_of(s * tok, 16), few), :].astype(jnp.bfloat16)
        return 0

    lax.fori_loop(0, nz, pack, 0)
    slot = cfg * nz + seq

    def share(peer):
        return pltpu.make_async_remote_copy(
            src_ref=vout.at[peer],
            dst_ref=vin.at[slot],
            send_sem=vsent,
            recv_sem=vrecv,
            device_id={"seq": peer, "cfg": 1},
            device_id_type=MESH,
        )

    def send_share(d, _):
        share(peer_at(d)).start()
        return 0

    lax.fori_loop(1, nz, send_share, 0)

    @pl.when(cfg == 0)
    def _():
        share(seq).start()
        pltpu.make_async_copy(vout, vout, vsent).wait()

    def greater(target_cfg):
        return blk < frames if target_cfg == 0 else blk >= frames - 2

    @pl.when(cfg == 1)
    def _():
        pltpu.make_async_copy(vout.at[seq], vin.at[slot], vrecv).start()
        pltpu.make_async_copy(vin, vin, vrecv).wait()
        guided = jnp.sum(vin[...].astype(jnp.float32), axis=0)
        noisy = jnp.concatenate([noisy_ref[0:few, :], noisy_ref[few:tok, :]], axis=1)
        scale = jnp.concatenate([std_ref[...]] * (2 * patch // ZCH), axis=1)
        shift = jnp.concatenate([mean_ref[...]] * (2 * patch // ZCH), axis=1)
        pixels = (noisy - NOISE_LEVEL * guided) * scale + shift
        pixels = jnp.concatenate([pixels[:, :patch], pixels[:, patch:]], axis=0).astype(jnp.bfloat16)

        entry = lax.broadcasted_iota(jnp.int32, (patch, 2 * patch), 0)
        lane = lax.broadcasted_iota(jnp.int32, (patch, 2 * patch), 1)
        half = patch // 2
        spread_pixels = []
        for p in range(2):
            place = (
                (entry // half == lane // patch)
                & (entry % half == lane % half)
                & ((lane // half) % 2 == p)
            ).astype(jnp.bfloat16)
            spread_pixels.append(jnp.dot(pixels, place, preferred_element_type=jnp.float32))
        spread_pixels = jnp.concatenate(spread_pixels, axis=0).astype(jnp.bfloat16)
        slots = order_ref[...] - (blk * nz + seq) * tok
        slots = jnp.concatenate([slots, slots], axis=1)
        row = lax.broadcasted_iota(jnp.int32, (ROW_PAD * nx, 2 * tok), 0)
        token = lax.broadcasted_iota(jnp.int32, (ROW_PAD * nx, 2 * tok), 1)
        x = row % ROW_PAD
        column = COLS_DEV * (row // ROW_PAD) - 1 + (x + 1) // 2 + token // tok
        inside = (x < 2 * COLS_DEV) & (column >= 0) & (column < COLS_DEV * nx)
        for i in range(2):
            select = (inside & (slots == column + i * COLS_DEV * nx)).astype(jnp.bfloat16)
            picked = jnp.dot(select, spread_pixels, preferred_element_type=jnp.float32)
            psend[:, :, i * 2 * patch : (i + 1) * 2 * patch] = picked.reshape(
                nx, ROW_PAD, 2 * patch
            ).astype(jnp.bfloat16)

        above = lax.rem(seq + nz - 1, nz)
        below = lax.rem(seq + 1, nz)
        pieces = (
            (1, pl.ds(2 * patch, 2 * patch), halo.at[blk, 0], below),
            (1, pl.ds(0, 2 * patch), halo.at[blk, 1], above),
            (0, pl.ds(0, 4 * patch), tile.at[blk], seq),
        )
        for c in range(2):

            @pl.when(greater(c))
            def _():
                def send_pieces(d, _):
                    far = nx // 2 - d // 2
                    b = lax.rem(blk + jnp.where(lax.rem(d, 2) == 1, far, nx - far), nx)
                    for kind, at, there, s in pieces:
                        pltpu.make_async_remote_copy(
                            src_ref=psend.at[b, :, at],
                            dst_ref=there,
                            send_sem=psent.at[c, kind],
                            recv_sem=precv.at[kind],
                            device_id={"seq": s, "blk": b, "cfg": c},
                            device_id_type=MESH,
                        ).start()
                    return 0

                lax.fori_loop(1, nx, send_pieces, 0)
                for kind, at, there, s in pieces:
                    if c == 1 and kind == 0:
                        pltpu.make_async_copy(psend.at[blk, :, at], there, precv.at[0]).start()
                    else:
                        pltpu.make_async_remote_copy(
                            src_ref=psend.at[blk, :, at],
                            dst_ref=there,
                            send_sem=psent.at[c, kind],
                            recv_sem=precv.at[kind],
                            device_id={"seq": s, "cfg": c},
                            device_id_type=MESH,
                        ).start()

    for c in range(2):

        @pl.when(cfg == c)
        def _():
            arrived = pl.ds(0, frames) if c == 0 else pl.ds(frames - 2, frames + 2)
            pltpu.make_async_copy(tile.at[arrived], tile.at[arrived], precv.at[0]).wait()
            pltpu.make_async_copy(halo.at[arrived], halo.at[arrived], precv.at[1]).wait()

    def line(g, _):
        frame = cfg * frames - 2 + g
        known = frame >= 0
        frame = jnp.maximum(frame, 0)
        upper = halo[frame, 0].astype(jnp.float32)[:, patch:]
        lower = halo[frame, 1].astype(jnp.float32)[:, :patch]
        upper = jnp.where(known & (seq > 0), upper, 0.0)
        lower = jnp.where(known & (seq < nz - 1), lower, 0.0)
        middle = jnp.where(known, tile[frame].astype(jnp.float32), 0.0)
        grid[g] = jnp.concatenate([upper, middle, lower], axis=1)
        return 0

    lax.fori_loop(0, frames + 2, line, 0)
    for f in range(frames):
        for y in range(4):
            for step_t in range(3):
                xcol[pl.ds((4 * f + y) * ROW_PAD, ROW_PAD), pl.ds(step_t * TAP_LANES, 3 * patch)] = grid[
                    f + step_t, :, pl.ds(y * patch, 3 * patch)
                ]
    odd = lax.broadcasted_iota(jnp.int32, xcol.shape, 0) % 2 == 1
    features = 0.0
    for parity in range(2):
        kept = jnp.where(odd if parity else ~odd, xcol[...], 0.0).astype(jnp.bfloat16)
        features = features + jnp.dot(kept, wexp[parity], preferred_element_type=jnp.float32)
    wide_x = 2 * COLS_DEV
    to = lax.broadcasted_iota(jnp.int32, (frames * wide_x * 4, xcol.shape[0]), 0)
    at = lax.broadcasted_iota(jnp.int32, (frames * wide_x * 4, xcol.shape[0]), 1)
    source = ((to // (4 * wide_x)) * 4 + to % 4) * ROW_PAD + (to // 4) % wide_x
    order = (source == at).astype(jnp.bfloat16)
    upper = features.astype(jnp.bfloat16)
    lower = (features - upper.astype(jnp.float32)).astype(jnp.bfloat16)
    final[...] = jnp.dot(order, upper, preferred_element_type=jnp.float32) + jnp.dot(
        order, lower, preferred_element_type=jnp.float32
    )
    for f in range(frames):
        for x in range(wide_x):
            out_ref[f, x] = final[pl.ds((f * wide_x + x) * 4, 4), :]

    @pl.when(cfg == 1)
    def _():
        sent = vout.at[pl.ds(0, nz - 1)]
        pltpu.make_async_copy(sent, sent, vsent).wait()
        for c in range(2):

            @pl.when(greater(c))
            def _():
                tiles = psend.at[pl.ds(0, nx - c)]
                pltpu.make_async_copy(tiles, tiles, psent.at[c, 0]).wait()
                pltpu.make_async_copy(psend, psend, psent.at[c, 1]).wait()

    for i, (_, whole, half) in enumerate(parcels):
        sent = whole if half == 1 else whole.at[pl.ds(0, whole.shape[0] - tok), :]
        pltpu.make_async_copy(sent, sent, zsend.at[i]).wait()
    for c in range(3):
        for step in range(1, hops + 1):
            for half in range(2):
                for way in range(2):
                    for piece in range(SPLIT if travels(way, step, half) else 0):
                        ring(c, way, step, half, piece).wait_send()


def local(
    queries,
    key_states,
    value_states,
    noisy_latents,
    patch_order,
    head_weight,
    latent_std,
    latent_mean,
    conv_weight,
    conv_bias,
):
    nz = lax.axis_size("seq")
    nx = lax.axis_size("blk")
    tok = queries.shape[1]
    rows = nz * tok
    patch = head_weight.shape[1]
    wide = conv_weight.shape[4]
    frames = nx // 2
    pixels = 4 * frames * ROW_PAD
    vmem = pl.BlockSpec(memory_space=pltpu.VMEM)
    features = pl.pallas_call(
        functools.partial(exchange_kernel, nz, nx),
        out_shape=jax.ShapeDtypeStruct((frames, 2 * COLS_DEV, 4, wide), jnp.float32),
        in_specs=[pl.BlockSpec(memory_space=pl.ANY)] * 5 + [vmem] * 4,
        out_specs=vmem,
        scratch_shapes=[
            pltpu.VMEM(queries.shape[1:], jnp.bfloat16),
            pltpu.VMEM(queries.shape[1:], jnp.bfloat16),
            pltpu.VMEM(queries.shape[1:], jnp.bfloat16),
            pltpu.VMEM((patch, head_weight.shape[0]), jnp.bfloat16),
            pltpu.VMEM((27 * ZCH, wide), jnp.bfloat16),
            pltpu.VMEM((nz, tok, 2 * patch), jnp.bfloat16),
            pltpu.VMEM((3, nx, rows, HDIM), jnp.bfloat16),
            pltpu.VMEM((2, rows, HDIM), jnp.bfloat16),
            pltpu.VMEM((nx, 2, patch + ONES, rows), jnp.bfloat16),
            pltpu.VMEM((2, 1, rows), jnp.float32),
            pltpu.VMEM((2, patch + ONES, rows), jnp.float32),
            pltpu.VMEM((rows, 2 * patch), jnp.float32),
            pltpu.VMEM((nz, tok // 2, 2 * patch), jnp.bfloat16),
            pltpu.VMEM((2 * nz, tok // 2, 2 * patch), jnp.bfloat16),
            pltpu.VMEM((nx, ROW_PAD, 4 * patch), jnp.bfloat16),
            pltpu.VMEM((nx, ROW_PAD, 4 * patch), jnp.bfloat16),
            pltpu.VMEM((nx, 2, ROW_PAD, 2 * patch), jnp.bfloat16),
            pltpu.VMEM((frames + 2, ROW_PAD, 6 * patch), jnp.float32),
            pltpu.VMEM((pixels, 3 * TAP_LANES), jnp.float32),
            pltpu.VMEM((2, 3 * TAP_LANES, wide), jnp.bfloat16),
            pltpu.VMEM((8 * frames * COLS_DEV, wide), jnp.float32),
            pltpu.SemaphoreType.DMA((8,)),
            pltpu.SemaphoreType.DMA((8,)),
            pltpu.SemaphoreType.DMA((3, 2, nx // 2, 2 * SPLIT)),
            pltpu.SemaphoreType.DMA((3, 2, nx // 2, 2 * SPLIT)),
            pltpu.SemaphoreType.DMA,
            pltpu.SemaphoreType.DMA,
            pltpu.SemaphoreType.DMA((2, 2)),
            pltpu.SemaphoreType.DMA((2,)),
            pltpu.SemaphoreType.DMA((5,)),
        ],
        compiler_params=pltpu.CompilerParams(
            collective_id=0, has_side_effects=True, vmem_limit_bytes=VMEM_LIMIT
        ),
    )(
        queries[0],
        key_states[0],
        value_states[0],
        head_weight.T,
        conv_weight.reshape(27 * ZCH, wide),
        noisy_latents,
        patch_order.reshape(1, tok),
        latent_std.reshape(1, ZCH),
        latent_mean.reshape(1, ZCH),
    )
    return (features + conv_bias).astype(jnp.bfloat16).transpose(0, 2, 1, 3)


def solution(mesh):
    in_specs = (
        P("cfg", ("prompt", "blk", "seq"), None),
        P("cfg", ("prompt", "blk", "seq"), None),
        P("cfg", ("prompt", "blk", "seq"), None),
        P(("prompt", "blk", "seq"), None),
        P(("prompt", "blk", "seq")),
        P(),
        P(),
        P(),
        P(),
        P(),
    )
    out_specs = P(("prompt", "cfg"), "seq", "blk", None)
    return jax.shard_map(local, mesh=mesh, in_specs=in_specs, out_specs=out_specs, check_vma=False)
```
